32 devices in a mesh: lon: 4 (over z), lat: 4 (over x, core), mem: 2 (over y).
Axes of the slice: x: 2, y: 2, z: 4, core: 2. Of those that a mesh axis runs over, the one named last changes fastest.
Arguments:
- tokens: bfloat16 [4, 8, 136, 24, 192], P('mem', None, 'lat', 'lon'), parts along dimension 0, may hold values from -6 to 6
- band_rows: int32 [4, 2], P('lat'), may hold values from 0 to 89, as said below
- down_gain: float32 [768], replicated, may hold values from 0.1 to 1.9
- down_shift: float32 [768], replicated, may hold values from -3 to 3
- down_weight: bfloat16 [768, 384], P(('lon', 'lat')), may hold values from -0.21875 to 0.21875
- up_weight: bfloat16 [384, 768], P(('lon', 'lat')), may hold values from -0.3125 to 0.3125
- up_gain: float32 [192], replicated, may hold values from 0.1 to 1.9
- up_shift: float32 [192], replicated, may hold values from -3 to 3
- mix_weight: bfloat16 [192, 192], replicated, may hold values from -0.4375 to 0.4375
Outputs:
- expanded: bfloat16 [4, 8, 136, 24, 192], P('mem', None, 'lat', 'lon'), parts along dimension 0
The draws below stay inside these ranges and needn't reach their ends.
There are 2 independent parts, one for each index of `mem`. The reference program is written for one: setup_inputs(seed, part) draws one part's arguments, and reference() takes and returns one part's arrays. A program takes and returns all parts, laid end to end along the dimension named above; an argument that names none is the same for every part. Nothing has to cross between parts.
Inputs may be any that keep to these rules, and one draw needn't show every extreme that they name: `band_rows`: row b holds band b's first latitude row and one past its last; the bands cover rows 0 to 88 in order without gaps; band 0 holds an odd number of rows and every other band an even number; each band holds at least 2 * (5) rows and at most 34, and some band other than band 0 holds exactly 34.
All inputs are finite; a program needn't handle non-finite values.
Results may differ from the reference program's by a relative error of at most 0.0062.
Values may be sent and summed in bfloat16 or wider, within the bound.
No kernel may reach another device: no remote copies, remote signals or barrier semaphores. Data moves between devices by JAX's collectives and lax.ppermute only.
A program may use at most 64 MiB of HBM per device.

```python
import jax
import jax.numpy as jnp
from jax import lax

C = 192
LEVELS = 8
MEMBERS = 2
BAND_ROWS = 22
BAND_ROW_SLOTS = 34
SLOTS = 136
LAT = 89
LON = 24
N_LAT = 4


def draw_band_rows(key, part):
    bands = N_LAT
    half_least = BAND_ROWS // 4
    slot_half = BAND_ROW_SLOTS // 2
    band_ids = jnp.arange(bands, dtype=jnp.int32)
    fullest = jax.random.randint(jax.random.fold_in(key, 11), (), 1, bands, dtype=jnp.int32)
    weights = jax.random.randint(jax.random.fold_in(key, 12), (bands,), 500, 1001, dtype=jnp.int32)
    order_keys = jax.random.permutation(jax.random.fold_in(key, 13), bands).astype(jnp.int32)
    sharing = band_ids != fullest
    weights = jnp.where(sharing, weights, 0)
    spare_halves = BAND_ROWS * bands // 2 - slot_half - (bands - 1) * half_least
    half_shares = spare_halves * weights // jnp.sum(weights)
    leftover = spare_halves - jnp.sum(half_shares)
    earlier = sharing[None, :] & (order_keys[None, :] < order_keys[:, None])
    ranking = jnp.sum(earlier.astype(jnp.int32), axis=1)
    extra_halves = (sharing & (ranking < leftover)).astype(jnp.int32)
    halves = jnp.where(band_ids == fullest, slot_half, half_least + half_shares + extra_halves)
    row_counts = (2 * halves + (band_ids == 0).astype(jnp.int32)).astype(jnp.int32)
    starts = jnp.cumsum(row_counts) - row_counts
    return jnp.stack([starts, starts + row_counts], axis=1).astype(jnp.int32)


def level_of(stream_key, extent, shards, smallest, top_value):
    def one(axis_at, parts):
        heights = jax.random.uniform(jax.random.fold_in(jax.random.fold_in(stream_key, 6), axis_at), (parts,), jnp.float32, smallest / len(shards), top_value / len(shards))
        return jnp.repeat(jnp.exp(heights), extent[axis_at] // parts).reshape((-1,) + (1,) * (len(extent) - axis_at - 1))

    level = one(*shards[0])
    for cut in shards[1:]:
        level = level * one(*cut)
    return level


def scatter_about(rng, dims, scale, most, cuts=(), kind=jnp.bfloat16):
    values = scale * jax.random.normal(rng, dims, jnp.float32)
    if cuts:
        values = values * level_of(rng, dims, cuts, -0.22, 0.18)
    return jnp.clip(values, -most, most).astype(kind)


def setup_inputs(seed: int = 0, part: int = 0) -> dict:
    streams_of = jax.random.split(jax.random.key(seed), 10)
    part_keys = jax.random.split(jax.random.fold_in(streams_of[9], part), 10)
    return {
        "tokens": scatter_about(part_keys[0], (MEMBERS, LEVELS, SLOTS, LON, C), 1.0, 6.0, ((2, 4), (3, 4))),
        "band_rows": draw_band_rows(jax.random.fold_in(streams_of[9], 71), part),
        "down_gain": jnp.clip(1.0 + 0.18 * jax.random.normal(streams_of[2], (4 * C,), jnp.float32), 0.1, 1.9),
        "down_shift": scatter_about(streams_of[3], (4 * C,), 0.5, 3.0, (), jnp.float32),
        "down_weight": scatter_about(streams_of[4], (4 * C, 2 * C), (4 * C) ** -0.5, 0.21875, ((0, 16),)),
        "up_weight": scatter_about(streams_of[5], (2 * C, 4 * C), (2 * C) ** -0.5, 0.3125, ((0, 16),)),
        "up_gain": jnp.clip(1.0 + 0.18 * jax.random.normal(streams_of[6], (C,), jnp.float32), 0.1, 1.9),
        "up_shift": scatter_about(streams_of[7], (C,), 0.5, 3.0, (), jnp.float32),
        "mix_weight": scatter_about(streams_of[8], (C, C), C ** -0.5, 0.4375),
    }


def normalize(values, scale_gain, bias_shift):
    average = lax.optimization_barrier(jnp.mean(values, axis=-1, keepdims=True))
    centred = values - average
    spread = lax.optimization_barrier(jnp.mean(centred * centred, axis=-1, keepdims=True))
    return centred * lax.rsqrt(spread + 1e-05) * scale_gain + bias_shift

def reference(tokens, band_rows, down_gain, down_shift, down_weight, up_weight, up_gain, up_shift, mix_weight):
    band_starts = band_rows[:, 0].astype(jnp.int32)
    band_ends = band_rows[:, 1].astype(jnp.int32)
    lat_rows = jnp.arange(LAT, dtype=jnp.int32)
    band_of = (lax.optimization_barrier(jnp.sum((lat_rows[:, None] >= band_starts[None, :]).astype(jnp.int32), axis=1)) - 1).astype(jnp.int32)
    source = (band_of * BAND_ROW_SLOTS + lat_rows - jnp.take(band_starts, band_of)).astype(jnp.int32)
    half_lat = (LAT + 1) // 2
    half_lon = LON // 2
    slot_ids = jnp.arange(SLOTS, dtype=jnp.int32)
    slot_band = (slot_ids // BAND_ROW_SLOTS).astype(jnp.int32)
    local_row = (slot_ids % BAND_ROW_SLOTS).astype(jnp.int32)
    live_rows = jnp.take(band_ends, slot_band) - jnp.take(band_starts, slot_band)
    global_row = (jnp.take(band_starts, slot_band) + local_row).astype(jnp.int32)
    is_live = local_row < live_rows
    safe_row = jnp.minimum(global_row, LAT - 1).astype(jnp.int32)

    def one_level(level_plane):
        field = jnp.take(level_plane, source, axis=0)
        field = jnp.pad(field, ((0, 1), (0, 0), (0, 0)))
        field = jnp.roll(field, -1, axis=1)
        blocks = field.reshape(half_lat, 2, half_lon, 2, C).transpose(0, 2, 3, 1, 4).reshape(half_lat * half_lon, 4 * C)
        merged_norm = normalize(blocks.astype(jnp.float32), down_gain, down_shift).astype(jnp.bfloat16)
        coarse = jnp.dot(merged_norm, down_weight, preferred_element_type=jnp.float32).astype(jnp.bfloat16)
        grown = jnp.dot(coarse, up_weight, preferred_element_type=jnp.float32)
        grown = grown.reshape(half_lat, half_lon, 2, 2, C).transpose(0, 2, 1, 3, 4).reshape(2 * half_lat, 2 * half_lon, C)[:LAT]
        grown = jnp.roll(grown, 1, axis=1)
        fine_norm = normalize(grown, up_gain, up_shift).astype(jnp.bfloat16)
        fine_out = jnp.dot(fine_norm.reshape(LAT * LON, C), mix_weight, preferred_element_type=jnp.float32)
        fine_out = fine_out.astype(jnp.bfloat16).reshape(LAT, LON, C)
        picked = jnp.take(fine_out, safe_row, axis=0)
        return jnp.where(is_live[:, None, None], picked, jnp.zeros_like(picked))
    planes = tokens.reshape(MEMBERS * LEVELS, SLOTS, LON, C)
    results = lax.map(one_level, planes)
    return results.reshape(MEMBERS, LEVELS, SLOTS, LON, C)
```

```python
import functools

import jax
import jax.numpy as jnp
from jax import lax
from jax.experimental import pallas as pl
from jax.experimental.pallas import tpu as pltpu
from jax.sharding import PartitionSpec as P


VMEM = pltpu.VMEM
SMEM = pltpu.SMEM
ANY = pl.ANY
EPS = 1e-05
LANES = 128


def shifted(block, axis, distance):
    n = lax.axis_size(axis)
    return lax.ppermute(block, axis, [(i, (i + distance) % n) for i in range(n)])


def passed_along(block, axis, distance):
    devices = range(lax.axis_size(axis))
    route = [(i, i + distance) for i in devices if i + distance in devices]
    return lax.ppermute(block, axis, route)


def pack_kernel(band_ref, tokens_ref, above_ref, below_ref, west_ref, east_ref, edge, sem):
    slots = tokens_ref.shape[1]
    columns = tokens_ref.shape[2]
    features = tokens_ref.shape[4]
    odd = lax.rem(band_ref[0, 0], 2)
    live = band_ref[0, 1] - band_ref[0, 0]
    copies = []
    for side, column in enumerate((0, columns - 1)):
        copy = pltpu.make_async_copy(
            tokens_ref.at[:, :, column], edge.at[side, :, pl.ds(odd, slots)], sem.at[side]
        )
        copy.start()
        copies.append(copy)
    for side, (column, out_ref) in enumerate(((0, west_ref), (columns - 1, east_ref))):
        copies[side].wait()
        edge[side, :, pl.ds(live + odd, 1)] = below_ref[:, pl.ds(column, 1)]

        @pl.when(odd == 1)
        def _():
            edge[side, :, pl.ds(0, 1)] = above_ref[:, pl.ds(column, 1)]

        both = edge[side].astype(jnp.float32)
        out_ref[:, 0] = both[0, :, :, :LANES].astype(jnp.bfloat16)
        out_ref[:, 1] = both[1, :, :, :LANES].astype(jnp.bfloat16)
        tails = jnp.concatenate([both[0, :, :, LANES:], both[1, :, :, LANES:]], axis=-1)
        out_ref[:, 2] = tails.astype(jnp.bfloat16)


def pack(band_rows, tokens, above, below):
    members, slots, columns, levels, features = tokens.shape
    rows = slots + 2
    out = jax.ShapeDtypeStruct((rows, 3, levels, LANES), jnp.bfloat16)
    return pl.pallas_call(
        pack_kernel,
        out_shape=(out, out),
        in_specs=[
            pl.BlockSpec(memory_space=SMEM),
            pl.BlockSpec(memory_space=ANY),
            pl.BlockSpec(memory_space=VMEM),
            pl.BlockSpec(memory_space=VMEM),
        ],
        out_specs=(pl.BlockSpec(memory_space=VMEM),) * 2,
        scratch_shapes=[
            pltpu.VMEM((2, members, rows, levels, features), jnp.bfloat16),
            pltpu.SemaphoreType.DMA((2,)),
        ],
        name="pack_edges",
    )(band_rows, tokens, above, below)


def main_kernel(
    band_ref,
    tokens_ref,
    above_ref,
    below_ref,
    west_ref,
    east_ref,
    gain_ref,
    shift_ref,
    down_ref,
    up_ref,
    up_gain_ref,
    up_shift_ref,
    mix_ref,
    out_ref,
    field,
    fine,
    sem,
):
    members, slots, columns, levels, features = tokens_ref.shape
    half_rows = slots // 2 + 1
    half_cols = columns // 2 + 1
    odd = lax.rem(band_ref[0, 0], 2)
    live = band_ref[0, 1] - band_ref[0, 0]
    load = pltpu.make_async_copy(
        tokens_ref, field.at[:, pl.ds(odd, slots), pl.ds(1, columns)], sem.at[0]
    )
    load.start()
    for column, edge_ref in ((0, west_ref), (columns + 1, east_ref)):
        for member in range(2):
            field[member, :, column, :, :LANES] = edge_ref[:, member]
        tails = edge_ref[:, 2].astype(jnp.float32)
        rest = features - LANES
        field[0, :, column, :, LANES:] = tails[..., :rest].astype(jnp.bfloat16)
        field[1, :, column, :, LANES:] = tails[..., rest:].astype(jnp.bfloat16)
    load.wait()
    field[:, pl.ds(live + odd, 1), pl.ds(1, columns)] = below_ref[...][:, None]

    @pl.when(odd == 1)
    def _():
        field[:, pl.ds(0, 1), pl.ds(1, columns)] = above_ref[...][:, None]

    pairs = field.reshape(members, half_rows, 2, half_cols, 2, levels, features)
    fine_pairs = fine.reshape(members, half_rows, 2, half_cols - 1, 2, levels, features)
    step = 6
    count = half_rows // step
    order = ((0, 0), (0, 1), (1, 0), (1, 1))

    def chunk(index, carry):
        base = index * step
        parts = [
            pairs[:, pl.ds(base, step), p, :, q].astype(jnp.float32).reshape(-1, features)
            for q, p in order
        ]
        total = parts[0] + parts[1] + parts[2] + parts[3]
        average = jnp.sum(total, axis=-1, keepdims=True) / (4 * features)
        parts = [part - average for part in parts]
        squares = parts[0] * parts[0]
        for part in parts[1:]:
            squares = squares + part * part
        spread = jnp.sum(squares, axis=-1, keepdims=True) / (4 * features)
        scale = lax.rsqrt(spread + EPS)
        coarse = None
        for k, part in enumerate(parts):
            normed = part * scale * gain_ref[k] + shift_ref[k]
            term = jnp.dot(
                normed.astype(jnp.bfloat16), down_ref[k], preferred_element_type=jnp.float32
            )
            coarse = term if coarse is None else coarse + term
        coarse = coarse.astype(jnp.bfloat16)
        for p in range(2):
            for q in range(2):
                grown = jnp.dot(coarse, up_ref[2 * p + q], preferred_element_type=jnp.float32)
                grown = grown.reshape(members, step, half_cols, levels, features)
                grown = grown[:, :, 1 - q : half_cols - q].reshape(-1, features)
                average = jnp.sum(grown, axis=-1, keepdims=True) / features
                grown = grown - average
                spread = jnp.sum(grown * grown, axis=-1, keepdims=True) / features
                normed = grown * lax.rsqrt(spread + EPS) * up_gain_ref[...] + up_shift_ref[...]
                mixed = jnp.dot(
                    normed.astype(jnp.bfloat16), mix_ref[...], preferred_element_type=jnp.float32
                )
                mixed = mixed.reshape(members, step, half_cols - 1, levels, features)
                fine_pairs[:, pl.ds(base, step), p, :, 1 - q] = mixed.astype(jnp.bfloat16)
        return carry

    lax.fori_loop(0, count, chunk, 0)

    def clear(row, carry):
        fine[:, pl.ds(row, 1)] = jnp.zeros((members, 1, columns, levels, features), jnp.bfloat16)
        return carry

    lax.fori_loop(live + odd, slots + 2, clear, 0)
    store = pltpu.make_async_copy(fine.at[:, pl.ds(odd, slots)], out_ref, sem.at[1])
    store.start()
    store.wait()


def merge_expand(
    band_rows, tokens, above, below, from_west, from_east, gain, shift, down, up, up_gain, up_shift, mix
):
    members, slots, columns, levels, features = tokens.shape
    rows = slots + 2
    vmem = pl.BlockSpec(memory_space=VMEM)
    any_space = pl.BlockSpec(memory_space=ANY)
    return pl.pallas_call(
        main_kernel,
        out_shape=jax.ShapeDtypeStruct(tokens.shape, jnp.bfloat16),
        in_specs=[pl.BlockSpec(memory_space=SMEM), any_space] + [vmem] * 11,
        out_specs=any_space,
        scratch_shapes=[
            pltpu.VMEM((members, rows, columns + 2, levels, features), jnp.bfloat16),
            pltpu.VMEM((members, rows, columns, levels, features), jnp.bfloat16),
            pltpu.SemaphoreType.DMA((2,)),
        ],
        name="merge_expand",
    )(band_rows, tokens, above, below, from_west, from_east, gain, shift, down, up, up_gain, up_shift, mix)


def gathered(down, up):
    lon, lat = lax.axis_size("lon"), lax.axis_size("lat")
    rows, narrow = down.shape
    up_rows, wide = up.shape
    shard = jnp.concatenate([down, up[:, :narrow], up[:, narrow:]], axis=0)
    if lat != 4 or up_rows % 8:
        whole = lax.all_gather(shard, ("lon", "lat"), axis=0)
        whole = whole.reshape(lon, lat, -1, narrow)
    else:
        here, band = lax.axis_index("lon"), lax.axis_index("lat")
        pieces = [(here, shard)]
        for k in range(1, lon):
            pieces.append(((here - k) % lon, shifted(shard, "lon", k)))
        line = jnp.zeros((lon,) + shard.shape, shard.dtype)
        for place, piece in pieces:
            line = lax.dynamic_update_index_in_dim(line, piece, place, 0)
        across = shifted(line, "lat", 2)
        half = jnp.stack([line, across])
        other = lax.ppermute(half, "lat", [(i, i ^ 1) for i in range(lat)])
        whole = jnp.zeros((lat,) + line.shape, shard.dtype)
        for place, piece in (
            (band, line),
            ((band + 2) % lat, across),
            (band ^ 1, other[0]),
            ((band ^ 1) ^ 2, other[1]),
        ):
            whole = lax.dynamic_update_index_in_dim(whole, piece, place, 0)
        whole = whole.transpose(1, 0, 2, 3)
    full_down = whole[:, :, :rows].reshape(-1, narrow)
    left = whole[:, :, rows : rows + up_rows].reshape(-1, narrow)
    right = whole[:, :, rows + up_rows :].reshape(-1, narrow)
    return full_down, left, right


def body(
    tokens, band_rows, down_gain, down_shift, down_weight, up_weight, up_gain, up_shift, mix_weight
):
    members, levels, slots, columns, features = tokens.shape
    block = tokens.transpose(0, 2, 3, 1, 4)
    live = band_rows[0, 1] - band_rows[0, 0]
    below = passed_along(block[:, 0], "lat", -1)
    above = passed_along(lax.dynamic_index_in_dim(block, live - 1, 1, False), "lat", 1)
    west, east = pack(band_rows, block, above, below)
    from_east = shifted(west, "lon", -1)
    from_west = shifted(east, "lon", 1)
    down, left, right = gathered(down_weight, up_weight)
    half = left.shape[-1] // 2
    up = jnp.stack([left[:, :half], left[:, half:], right[:, :half], right[:, half:]])
    out = merge_expand(
        band_rows,
        block,
        above,
        below,
        from_west,
        from_east,
        down_gain.reshape(4, 1, features),
        down_shift.reshape(4, 1, features),
        down.reshape(4, features, -1),
        up,
        up_gain.reshape(1, features),
        up_shift.reshape(1, features),
        mix_weight,
    )
    return out.transpose(0, 3, 1, 2, 4)


def solution(mesh):
    return jax.shard_map(
        body,
        mesh=mesh,
        in_specs=(
            P("mem", None, "lat", "lon", None),
            P("lat", None),
            P(),
            P(),
            P(("lon", "lat"), None),
            P(("lon", "lat"), None),
            P(),
            P(),
            P(),
        ),
        out_specs=P("mem", None, "lat", "lon", None),
        check_vma=False,
    )
```

```python
import functools

import jax
import jax.numpy as jnp
from jax import lax
from jax.experimental import pallas as pl
from jax.experimental.pallas import tpu as pltpu
from jax.sharding import PartitionSpec as P


EPS = 1e-05
F32 = jnp.float32
BF16 = jnp.bfloat16
VMEM = pl.BlockSpec(memory_space=pltpu.VMEM)
SMEM = pl.BlockSpec(memory_space=pltpu.SMEM)
ANY = pl.BlockSpec(memory_space=pl.ANY)
ORDER = ((0, 0), (0, 1), (1, 0), (1, 1))


def shifted(block, axis, distance):
    n = lax.axis_size(axis)
    return lax.ppermute(block, axis, [(i, (i + distance) % n) for i in range(n)])


def passed_along(block, axis, distance):
    devices = range(lax.axis_size(axis))
    route = [(i, i + distance) for i in devices if i + distance in devices]
    return lax.ppermute(block, axis, route)


def swapped(block, axis, partner):
    n = lax.axis_size(axis)
    return lax.ppermute(block, axis, [(i, partner(i)) for i in range(n)])


def band(band_ref):
    odd = lax.rem(band_ref[0, 0], 2)
    return odd, band_ref[0, 1] - band_ref[0, 0]


def room(mebibytes):
    return pltpu.CompilerParams(vmem_limit_bytes=mebibytes * 2**20)


def cost(flops, moved):
    return pl.CostEstimate(flops=flops, bytes_accessed=moved, transcendentals=0)


def shard_kernel(down_ref, up_ref, shard_ref, sem):
    tiles = down_ref.shape[0]
    up_tiles, _, wide = up_ref.shape
    half = wide // 2
    copies = [
        pltpu.make_async_copy(down_ref, shard_ref.at[:tiles], sem.at[0]),
        pltpu.make_async_copy(
            up_ref.at[:, :, :half], shard_ref.at[tiles : tiles + up_tiles], sem.at[1]
        ),
        pltpu.make_async_copy(up_ref.at[:, :, half:], shard_ref.at[tiles + up_tiles :], sem.at[2]),
    ]
    for copy in copies:
        copy.start()
    for copy in copies:
        copy.wait()


def shard_of(down, up):
    tiles, up_tiles = down.shape[0] // 8, up.shape[0] // 8
    return pl.pallas_call(
        shard_kernel,
        out_shape=jax.ShapeDtypeStruct((tiles + 2 * up_tiles, 8, down.shape[1]), BF16),
        in_specs=[ANY, ANY],
        out_specs=VMEM,
        scratch_shapes=[pltpu.SemaphoreType.DMA((3,))],
        compiler_params=room(1),
        name="shard",
    )(down.reshape(tiles, 8, -1), up.reshape(up_tiles, 8, -1))


def joined(pair):
    return jnp.concatenate([pair[0].astype(F32), pair[1].astype(F32)], axis=-1).astype(BF16)


def edges_kernel(band_ref, tokens_ref, first_ref, last_ref, west_ref, east_ref, rows, cols, sem):
    slots, columns = tokens_ref.shape[1:3]
    odd, live = band(band_ref)
    copies = [
        pltpu.make_async_copy(tokens_ref.at[:, 0], rows.at[0], sem.at[0]),
        pltpu.make_async_copy(tokens_ref.at[:, live - 1], rows.at[1], sem.at[1]),
        pltpu.make_async_copy(tokens_ref.at[:, :, 0], cols.at[0], sem.at[2]),
        pltpu.make_async_copy(tokens_ref.at[:, :, columns - 1], cols.at[1], sem.at[3]),
    ]
    for copy in copies:
        copy.start()
    for side, out_ref in enumerate((first_ref, last_ref)):
        copies[side].wait()
        out_ref[...] = joined(rows[side])
    for side, out_ref in enumerate((west_ref, east_ref)):
        copies[2 + side].wait()
        out_ref[pl.ds(odd, slots)] = joined(cols[side])


def edges_of(band_rows, tokens):
    members, slots, columns, levels, features = tokens.shape
    row = jax.ShapeDtypeStruct((columns, levels, members * features), BF16)
    col = jax.ShapeDtypeStruct((slots + 2, levels, members * features), BF16)
    return pl.pallas_call(
        edges_kernel,
        out_shape=(row, row, col, col),
        in_specs=[SMEM, ANY],
        out_specs=(VMEM,) * 4,
        scratch_shapes=[
            pltpu.VMEM((2, members, columns, levels, features), BF16),
            pltpu.VMEM((2, members, slots, levels, features), BF16),
            pltpu.SemaphoreType.DMA((4,)),
        ],
        compiler_params=room(4),
        name="edges",
    )(band_rows, tokens)


def corners_kernel(band_ref, above_ref, below_ref, west_in, east_in, west_ref, east_ref):
    odd, live = band(band_ref)
    columns = above_ref.shape[0]
    west_ref[...] = west_in[...]
    east_ref[...] = east_in[...]
    for column, out_ref in ((0, west_ref), (columns - 1, east_ref)):
        out_ref[pl.ds(live + odd, 1)] = below_ref[pl.ds(column, 1)]

        @pl.when(odd == 1)
        def _():
            out_ref[pl.ds(0, 1)] = above_ref[pl.ds(column, 1)]


def with_corners(band_rows, above, below, west, east):
    out = jax.ShapeDtypeStruct(west.shape, BF16)
    return pl.pallas_call(
        corners_kernel,
        out_shape=(out, out),
        in_specs=[SMEM] + [VMEM] * 4,
        out_specs=(VMEM,) * 2,
        compiler_params=room(1),
        name="corners",
    )(band_rows, above, below, west, east)


def merge_normed(parts, gain_ref, shift_ref):
    features = parts[0].shape[-1]
    total = parts[0] + parts[1] + parts[2] + parts[3]
    average = jnp.sum(total, axis=-1, keepdims=True) / (4 * features)
    parts = [part - average for part in parts]
    squares = parts[0] * parts[0]
    for part in parts[1:]:
        squares = squares + part * part
    spread = jnp.sum(squares, axis=-1, keepdims=True) / (4 * features)
    scale = lax.rsqrt(spread + EPS)
    return [
        (part * scale * gain_ref[k] + shift_ref[k]).astype(BF16) for k, part in enumerate(parts)
    ]


def fine_rows(grown, gain_ref, shift_ref, mix_ref):
    features = grown.shape[-1]
    average = jnp.sum(grown, axis=-1, keepdims=True) / features
    grown = grown - average
    spread = jnp.sum(grown * grown, axis=-1, keepdims=True) / features
    normed = grown * lax.rsqrt(spread + EPS) * gain_ref[...] + shift_ref[...]
    return jnp.dot(normed.astype(BF16), mix_ref[...], preferred_element_type=F32)


def cleared(band_ref, fine):
    odd, live = band(band_ref)
    members, rows = fine.shape[:2]

    def clear(row, carry):
        fine[:, pl.ds(row, 1)] = jnp.zeros((members, 1) + fine.shape[2:], BF16)
        return carry

    lax.fori_loop(live + odd, rows, clear, 0)
    return odd


def inner_norm_kernel(
    band_ref, tokens_ref, above_ref, below_ref, gain_ref, shift_ref, out_ref, field, sem
):
    members, slots, columns, levels, features = tokens_ref.shape
    half_rows, inner = slots // 2 + 1, columns - 2
    odd, live = band(band_ref)
    load = pltpu.make_async_copy(
        tokens_ref.at[:, :, pl.ds(1, inner)], field.at[:, pl.ds(odd, slots)], sem
    )
    load.start()
    load.wait()
    for member in range(members):
        lanes = slice(member * features, (member + 1) * features)

        @pl.when(odd == 1)
        def _():
            row = above_ref[1 : columns - 1].astype(F32)[..., lanes]
            field[member, pl.ds(0, 1)] = row.astype(BF16)[None]

        row = below_ref[1 : columns - 1].astype(F32)[..., lanes]
        field[member, pl.ds(live + odd, 1)] = row.astype(BF16)[None]
    pairs = field.reshape(members, half_rows, 2, inner // 2, 2, levels, features)
    step = out_ref.shape[2] // (members * inner // 2 * levels)

    def chunk(index, carry):
        parts = [
            pairs[:, pl.ds(index * step, step), p, :, q].astype(F32).reshape(-1, features)
            for q, p in ORDER
        ]
        for k, part in enumerate(merge_normed(parts, gain_ref, shift_ref)):
            out_ref[index, k] = part
        return carry

    lax.fori_loop(0, out_ref.shape[0], chunk, 0)


def steps_of(half_rows):
    return max(step for step in range(1, 7) if half_rows % step == 0)


def inner_norm(band_rows, tokens, above, below, gain, shift):
    members, slots, columns, levels, features = tokens.shape
    half_rows, inner = slots // 2 + 1, columns - 2
    step = steps_of(half_rows)
    rows = step * members * inner // 2 * levels
    return pl.pallas_call(
        inner_norm_kernel,
        out_shape=jax.ShapeDtypeStruct((half_rows // step, 4, rows, features), BF16),
        in_specs=[SMEM, ANY] + [VMEM] * 4,
        out_specs=VMEM,
        scratch_shapes=[
            pltpu.VMEM((members, slots + 2, inner, levels, features), BF16),
            pltpu.SemaphoreType.DMA,
        ],
        cost_estimate=cost(10**9, 10**6),
        compiler_params=room(10),
        name="inner_norm",
    )(band_rows, tokens, above, below, gain, shift)


def inner_kernel(
    band_ref, normed_ref, down_ref, up_ref, gain_ref, shift_ref, mix_ref, out_ref, fine, sem
):
    members, slots, columns, levels, features = out_ref.shape
    half_rows, inner = slots // 2 + 1, columns - 2
    count = normed_ref.shape[0]
    step = half_rows // count
    pairs = fine.reshape(members, half_rows, 2, inner // 2, 2, levels, features)

    def chunk(index, carry):
        coarse = None
        for k in range(4):
            term = jnp.dot(normed_ref[index, k], down_ref[k], preferred_element_type=F32)
            coarse = term if coarse is None else coarse + term
        coarse = coarse.astype(BF16)
        for p in range(2):
            both = jnp.dot(coarse, up_ref[p], preferred_element_type=F32)
            for q in range(2):
                grown = both[:, q * features : (q + 1) * features]
                mixed = fine_rows(grown, gain_ref, shift_ref, mix_ref)
                mixed = mixed.reshape(members, step, inner // 2, levels, features)
                pairs[:, pl.ds(index * step, step), p, :, q] = mixed.astype(BF16)
        return carry

    lax.fori_loop(0, count, chunk, 0)
    odd = cleared(band_ref, fine)
    store = pltpu.make_async_copy(
        fine.at[:, pl.ds(odd, slots)], out_ref.at[:, :, pl.ds(1, inner)], sem
    )
    store.start()
    store.wait()


def inner_of(band_rows, normed, down, up, gain, shift, mix, shape):
    members, slots, columns, levels, features = shape
    return pl.pallas_call(
        inner_kernel,
        out_shape=jax.ShapeDtypeStruct(shape, BF16),
        in_specs=[SMEM] + [VMEM] * 6,
        out_specs=ANY,
        scratch_shapes=[
            pltpu.VMEM((members, slots + 2, columns - 2, levels, features), BF16),
            pltpu.SemaphoreType.DMA,
        ],
        cost_estimate=cost(4 * 10**9, 10**6),
        compiler_params=room(16),
        name="inner",
    )(band_rows, normed, down, up, gain, shift, mix)


def outer_kernel(
    band_ref,
    from_west_ref,
    west_ref,
    east_ref,
    from_east_ref,
    gain_ref,
    shift_ref,
    down_ref,
    up_ref,
    up_gain_ref,
    up_shift_ref,
    mix_ref,
    partial_ref,
    out_ref,
    fine,
    sem,
):
    del partial_ref
    members, slots, columns, levels, features = out_ref.shape
    half_rows = slots // 2 + 1
    odd, _ = band(band_ref)
    copies = []
    for side, refs in enumerate(((from_west_ref, west_ref), (east_ref, from_east_ref))):
        parts = []
        for q, p in ORDER:
            column = refs[q].reshape(half_rows, 2, levels, members * features)[:, p]
            column = column.astype(F32).reshape(-1, members * features)
            parts.append(
                jnp.concatenate(
                    [column[:, m * features : (m + 1) * features] for m in range(members)], axis=0
                )
            )
        coarse = None
        for k, part in enumerate(merge_normed(parts, gain_ref, shift_ref)):
            term = jnp.dot(part, down_ref[k], preferred_element_type=F32)
            coarse = term if coarse is None else coarse + term
        coarse = coarse.astype(BF16)
        q = 1 - side
        for p in range(2):
            weight = up_ref[p, :, q * features : (q + 1) * features]
            grown = jnp.dot(coarse, weight, preferred_element_type=F32)
            mixed = fine_rows(grown, up_gain_ref, up_shift_ref, mix_ref)
            mixed = mixed.reshape(members, half_rows, levels, features)
            view = fine.at[side].reshape(members, half_rows, 2, levels, features)
            view[:, :, p] = mixed.astype(BF16)
        cleared(band_ref, fine.at[side])
        copy = pltpu.make_async_copy(
            fine.at[side, :, pl.ds(odd, slots)],
            out_ref.at[:, :, side * (columns - 1)],
            sem.at[side],
        )
        copy.start()
        copies.append(copy)
    for copy in copies:
        copy.wait()


def outer_of(band_rows, sides, gain, shift, down, up, up_gain, up_shift, mix, partial):
    members, slots, columns, levels, features = partial.shape
    return pl.pallas_call(
        outer_kernel,
        out_shape=jax.ShapeDtypeStruct(partial.shape, BF16),
        in_specs=[SMEM] + [VMEM] * 11 + [ANY],
        out_specs=ANY,
        scratch_shapes=[
            pltpu.VMEM((2, members, slots + 2, levels, features), BF16),
            pltpu.SemaphoreType.DMA((2,)),
        ],
        input_output_aliases={12: 0},
        cost_estimate=cost(3 * 10**9, 10**6),
        compiler_params=room(12),
        name="outer",
    )(band_rows, *sides, gain, shift, down, up, up_gain, up_shift, mix, partial)


def assemble_kernel(*refs):
    pieces, (down_ref, up_ref) = refs[:-2], refs[-2:]
    lon, lat, tiles = down_ref.shape[:3]
    up_tiles = up_ref.shape[3]
    here, place = lax.axis_index("lon"), lax.axis_index("lat")
    own, z1, z2, z3, core, across, across12, across3, rest, last = pieces
    far = lat - 1 - place
    beside = lax.bitwise_xor(place, 1)
    beside_far = lat - 1 - beside
    n = tiles + 2 * up_tiles
    table = [
        (own, 0, 0, place),
        (z1, 0, 1, place),
        (z2, 0, 2, place),
        (z3, 0, 3, place),
        (core, 0, 0, beside),
        (across, 0, 0, far),
        (across12, 0, 1, far),
        (across12, n, 2, far),
        (across3, 0, 3, far),
        (rest, 0, 1, beside),
        (rest, n, 2, beside),
        (rest, 2 * n, 3, beside),
        (rest, 3 * n, 0, beside_far),
        (rest, 4 * n, 1, beside_far),
        (rest, 5 * n, 2, beside_far),
        (last, 0, 3, beside_far),
    ]
    for ref, at, hop, row in table:
        source = lax.bitwise_xor(here, hop)
        down_ref[source, row] = ref[at : at + tiles]
        up_ref[0, source, row] = ref[at + tiles : at + tiles + up_tiles]
        up_ref[1, source, row] = ref[at + tiles + up_tiles : at + n]


def fast_weights(down, up, first, last):
    lon, lat = lax.axis_size("lon"), lax.axis_size("lat")
    tiles, up_tiles = down.shape[0] // 8, up.shape[0] // 8
    place = lax.axis_index("lat")
    with jax.named_scope("shard"):
        shard = shard_of(down, up)
    mirror = lambda i: lat - 1 - i
    with jax.named_scope("z2"):
        z2 = swapped(shard, "lon", lambda i: i ^ 2)
    with jax.named_scope("z3"):
        z3 = swapped(shard, "lon", lambda i: i ^ 3)
    with jax.named_scope("z1"):
        z1 = swapped(shard, "lon", lambda i: i ^ 1)
    even = place % 2 == 0
    with jax.named_scope("core"):
        rows = jnp.where(even, last, first)
        core = swapped(jnp.concatenate([shard, rows]), "lat", lambda i: i ^ 1)
    with jax.named_scope("x"):
        rows = jnp.where(even, first, last)
        across = swapped(jnp.concatenate([shard, rows]), "lat", mirror)
    n = shard.shape[0]
    core_rows, across_rows = core[n:], across[n:]
    below = jnp.where(even, core_rows, across_rows)
    below = jnp.where(place == lat - 1, jnp.zeros_like(below), below)
    above = jnp.where(even, across_rows, core_rows)
    with jax.named_scope("x12"):
        across12 = swapped(jnp.concatenate([z1, z2]), "lat", mirror)
    with jax.named_scope("x3"):
        across3 = swapped(z3, "lat", mirror)
    with jax.named_scope("rest"):
        rest = jnp.concatenate([z1, z2, z3, across[:n], across12])
        rest = swapped(rest, "lat", lambda i: i ^ 1)
    with jax.named_scope("last"):
        final = swapped(across3, "lat", lambda i: i ^ 1)
    down, up = pl.pallas_call(
        assemble_kernel,
        out_shape=(
            jax.ShapeDtypeStruct((lon, lat, tiles, 8, down.shape[1]), BF16),
            jax.ShapeDtypeStruct((2, lon, lat, up_tiles, 8, down.shape[1]), BF16),
        ),
        in_specs=[VMEM] * 10,
        out_specs=(VMEM,) * 2,
        compiler_params=room(6),
        name="assemble",
    )(shard, z1, z2, z3, core, across, across12, across3, rest, final)
    return down, up, above, below


def plain_weights(down, up, first, last):
    below = passed_along(first, "lat", -1)
    above = passed_along(last, "lat", 1)
    rows, half = up.shape[0], up.shape[1] // 2
    shard = jnp.concatenate([down, up[:, :half], up[:, half:]], axis=0)
    whole = lax.all_gather(shard, ("lon", "lat"), axis=0)
    n = down.shape[0]
    up = jnp.stack([whole[:, n : n + rows], whole[:, n + rows :]])
    return whole[:, :n], up, above, below


def body(
    tokens, band_rows, down_gain, down_shift, down_weight, up_weight, up_gain, up_shift, mix_weight
):
    members, levels, slots, columns, features = tokens.shape
    lon, lat = lax.axis_size("lon"), lax.axis_size("lat")
    block = tokens.transpose(0, 2, 3, 1, 4)
    with jax.named_scope("edges"):
        first, last, west, east = edges_of(band_rows, block)
    plain = lon != 4 or lat != 4 or down_weight.shape[0] % 8 or up_weight.shape[0] % 8
    weights = plain_weights if plain else fast_weights
    down, up, above, below = weights(down_weight, up_weight, first, last)
    narrow = down_weight.shape[1]
    down = down.reshape(4, features, narrow)
    up = up.reshape(2, narrow, narrow)
    with jax.named_scope("corners"):
        west, east = with_corners(band_rows, above, below, west, east)
    with jax.named_scope("from_east"):
        from_east = shifted(west, "lon", -1)
    with jax.named_scope("from_west"):
        from_west = shifted(east, "lon", 1)
    gain, shift = down_gain.reshape(4, 1, features), down_shift.reshape(4, 1, features)
    fine_gain, fine_shift = up_gain.reshape(1, features), up_shift.reshape(1, features)
    with jax.named_scope("inner_norm"):
        normed = inner_norm(band_rows, block, above, below, gain, shift)
    with jax.named_scope("inner"):
        out = inner_of(
            band_rows, normed, down, up, fine_gain, fine_shift, mix_weight, block.shape
        )
    with jax.named_scope("outer"):
        out = outer_of(
            band_rows,
            (from_west, west, east, from_east),
            gain,
            shift,
            down,
            up,
            fine_gain,
            fine_shift,
            mix_weight,
            out,
        )
    return out.transpose(0, 3, 1, 2, 4)


def solution(mesh):
    return jax.shard_map(
        body,
        mesh=mesh,
        in_specs=(
            P("mem", None, "lat", "lon", None),
            P("lat", None),
            P(),
            P(),
            P(("lon", "lat"), None),
            P(("lon", "lat"), None),
            P(),
            P(),
            P(),
        ),
        out_specs=P("mem", None, "lat", "lon", None),
        check_vma=False,
    )
```

```python
import functools

import jax
import jax.numpy as jnp
from jax import lax
from jax.experimental import pallas as pl
from jax.experimental.pallas import tpu as pltpu
from jax.sharding import PartitionSpec as P


EPS = 1e-05
LANES = 128
PAD = 64
F32 = jnp.float32
BF16 = jnp.bfloat16
VMEM = pl.BlockSpec(memory_space=pltpu.VMEM)
SMEM = pl.BlockSpec(memory_space=pltpu.SMEM)
ANY = pl.BlockSpec(memory_space=pl.ANY)
ORDER = ((0, 0), (0, 1), (1, 0), (1, 1))


def shifted(block, axis, distance):
    n = lax.axis_size(axis)
    return lax.ppermute(block, axis, [(i, (i + distance) % n) for i in range(n)])


def passed_along(block, axis, distance):
    devices = range(lax.axis_size(axis))
    route = [(i, i + distance) for i in devices if i + distance in devices]
    return lax.ppermute(block, axis, route)


def swapped(block, axis, partner):
    n = lax.axis_size(axis)
    return lax.ppermute(block, axis, [(i, partner(i)) for i in range(n)])


def band(band_ref):
    odd = lax.rem(band_ref[0, 0], 2)
    return odd, band_ref[0, 1] - band_ref[0, 0]


def room(mebibytes):
    return pltpu.CompilerParams(vmem_limit_bytes=mebibytes * 2**20)


def cost(flops, moved):
    return pl.CostEstimate(flops=flops, bytes_accessed=moved, transcendentals=0)


def centred(weight, features):
    blocks = []
    for start in range(0, weight.shape[-1], features):
        block = weight[..., start : start + features].astype(F32)
        blocks.append(block - jnp.mean(block, axis=-1, keepdims=True))
    return jnp.concatenate(blocks, axis=-1).astype(BF16)


def shard_kernel(features, down_ref, up_ref, shard_ref):
    tiles = down_ref.shape[0]
    up_tiles, _, wide = up_ref.shape
    half = wide // 2
    shard_ref[:tiles] = down_ref[...]
    up = centred(up_ref[...], features)
    shard_ref[tiles : tiles + up_tiles] = up[..., :half]
    shard_ref[tiles + up_tiles :] = up[..., half:]


def shard_of(down, up, features):
    tiles, up_tiles = down.shape[0] // 8, up.shape[0] // 8
    return pl.pallas_call(
        functools.partial(shard_kernel, features),
        out_shape=jax.ShapeDtypeStruct((tiles + 2 * up_tiles, 8, down.shape[1]), BF16),
        in_specs=[VMEM, VMEM],
        out_specs=VMEM,
        compiler_params=room(1),
        name="shard",
    )(down.reshape(tiles, 8, -1), up.reshape(up_tiles, 8, -1))


def joined(pair):
    return jnp.concatenate([pair[0].astype(F32), pair[1].astype(F32)], axis=-1).astype(BF16)


def edges_kernel(band_ref, tokens_ref, first_ref, last_ref, west_ref, east_ref, rows, cols, sem):
    slots, columns = tokens_ref.shape[1:3]
    odd, live = band(band_ref)
    copies = [
        pltpu.make_async_copy(tokens_ref.at[:, 0], rows.at[0], sem.at[0]),
        pltpu.make_async_copy(tokens_ref.at[:, live - 1], rows.at[1], sem.at[1]),
        pltpu.make_async_copy(tokens_ref.at[:, :, 0], cols.at[0], sem.at[2]),
        pltpu.make_async_copy(tokens_ref.at[:, :, columns - 1], cols.at[1], sem.at[3]),
    ]
    for copy in copies:
        copy.start()
    for side, out_ref in enumerate((first_ref, last_ref)):
        copies[side].wait()
        out_ref[...] = joined(rows[side])
    for side, out_ref in enumerate((west_ref, east_ref)):
        copies[2 + side].wait()
        out_ref[pl.ds(odd, slots)] = joined(cols[side])


def edges_of(band_rows, tokens):
    members, slots, columns, levels, features = tokens.shape
    row = jax.ShapeDtypeStruct((columns, levels, members * features), BF16)
    col = jax.ShapeDtypeStruct((slots + 2, levels, members * features), BF16)
    return pl.pallas_call(
        edges_kernel,
        out_shape=(row, row, col, col),
        in_specs=[SMEM, ANY],
        out_specs=(VMEM,) * 4,
        scratch_shapes=[
            pltpu.VMEM((2, members, columns, levels, features), BF16),
            pltpu.VMEM((2, members, slots, levels, features), BF16),
            pltpu.SemaphoreType.DMA((4,)),
        ],
        compiler_params=room(4),
        name="edges",
    )(band_rows, tokens)


def corners_kernel(band_ref, above_ref, below_ref, west_in, east_in, west_ref, east_ref):
    odd, live = band(band_ref)
    columns = above_ref.shape[0]
    west_ref[...] = west_in[...]
    east_ref[...] = east_in[...]
    for column, out_ref in ((0, west_ref), (columns - 1, east_ref)):
        out_ref[pl.ds(live + odd, 1)] = below_ref[pl.ds(column, 1)]

        @pl.when(odd == 1)
        def _():
            out_ref[pl.ds(0, 1)] = above_ref[pl.ds(column, 1)]


def with_corners(band_rows, above, below, west, east):
    out = jax.ShapeDtypeStruct(west.shape, BF16)
    return pl.pallas_call(
        corners_kernel,
        out_shape=(out, out),
        in_specs=[SMEM] + [VMEM] * 4,
        out_specs=(VMEM,) * 2,
        compiler_params=room(1),
        name="corners",
    )(band_rows, above, below, west, east)


def merge_normed(parts, gain_ref, shift_ref):
    features = parts[0].shape[-1]
    total = parts[0] + parts[1] + parts[2] + parts[3]
    average = jnp.sum(total, axis=-1, keepdims=True) / (4 * features)
    parts = [part - average for part in parts]
    squares = parts[0] * parts[0]
    for part in parts[1:]:
        squares = squares + part * part
    spread = jnp.sum(squares, axis=-1, keepdims=True) / (4 * features)
    scale = lax.rsqrt(spread + EPS)
    return [
        (part * scale * gain_ref[k] + shift_ref[k]).astype(BF16) for k, part in enumerate(parts)
    ]


def group_sums(width, features):
    shape = (width, 2 * LANES)
    first = lax.broadcasted_iota(jnp.int32, shape, 0) < features
    low = lax.broadcasted_iota(jnp.int32, shape, 1) < LANES
    return jnp.where(first == low, 1.0, 0.0).astype(BF16)


def blended(low, high, rest):
    lane = lax.broadcasted_iota(jnp.int32, low.shape, 1)
    return jnp.concatenate([low, jnp.where(lane < rest, low, high), high], axis=-1)


def window(rows, q):
    return rows[:, q * LANES : q * LANES + 2 * LANES]


def mixed_pair(grown, sums, gain_ref, shift_ref, mix_ref, features):
    squares = (grown * grown).astype(BF16)
    spread = jnp.dot(squares, sums, preferred_element_type=F32)
    scale = lax.rsqrt(spread * (1.0 / features) + EPS)
    scale = blended(scale[:, :LANES], scale[:, LANES:], features - LANES)
    normed = (grown * scale * gain_ref[...] + shift_ref[...]).astype(BF16)
    return [padded_dot(window(normed, q), mix_ref, q) for q in range(2)]


def padded_dot(rows, weight_ref, q):
    start = (1 - q) * PAD
    weight = weight_ref[start : start + 2 * LANES]
    return jnp.dot(rows, weight, preferred_element_type=F32)


def cleared(band_ref, fine):
    odd, live = band(band_ref)
    members, rows = fine.shape[:2]

    def clear(row, carry):
        fine[:, pl.ds(row, 1)] = jnp.zeros((members, 1) + fine.shape[2:], BF16)
        return carry

    lax.fori_loop(live + odd, rows, clear, 0)
    return odd


def inner_norm_kernel(
    band_ref, tokens_ref, above_ref, below_ref, gain_ref, shift_ref, out_ref, field, sem
):
    members, slots, columns, levels, features = tokens_ref.shape
    half_rows, inner = slots // 2 + 1, columns - 2
    odd, live = band(band_ref)
    load = pltpu.make_async_copy(
        tokens_ref.at[:, :, pl.ds(1, inner)], field.at[:, pl.ds(odd, slots)], sem
    )
    load.start()
    load.wait()
    for member in range(members):
        lanes = slice(member * features, (member + 1) * features)

        @pl.when(odd == 1)
        def _():
            row = above_ref[1 : columns - 1].astype(F32)[..., lanes]
            field[member, pl.ds(0, 1)] = row.astype(BF16)[None]

        row = below_ref[1 : columns - 1].astype(F32)[..., lanes]
        field[member, pl.ds(live + odd, 1)] = row.astype(BF16)[None]
    pairs = field.reshape(members, half_rows, 2, inner // 2, 2, levels, features)
    step = out_ref.shape[1] // (members * inner // 2 * levels)

    def chunk(index, carry):
        parts = [
            pairs[:, pl.ds(index * step, step), p, :, q].astype(F32).reshape(-1, features)
            for q, p in ORDER
        ]
        out_ref[index] = jnp.concatenate(merge_normed(parts, gain_ref, shift_ref), axis=-1)
        return carry

    lax.fori_loop(0, out_ref.shape[0], chunk, 0)


def steps_of(half_rows):
    return max(step for step in range(1, 7) if half_rows % step == 0)


def inner_norm(band_rows, tokens, above, below, gain, shift):
    members, slots, columns, levels, features = tokens.shape
    half_rows, inner = slots // 2 + 1, columns - 2
    step = steps_of(half_rows)
    rows = step * members * inner // 2 * levels
    return pl.pallas_call(
        inner_norm_kernel,
        out_shape=jax.ShapeDtypeStruct((half_rows // step, rows, 4 * features), BF16),
        in_specs=[SMEM, ANY] + [VMEM] * 4,
        out_specs=VMEM,
        scratch_shapes=[
            pltpu.VMEM((members, slots + 2, inner, levels, features), BF16),
            pltpu.SemaphoreType.DMA,
        ],
        cost_estimate=cost(10**9, 10**6),
        compiler_params=room(10),
        name="inner_norm",
    )(band_rows, tokens, above, below, gain, shift)


def inner_kernel(
    band_ref, normed_ref, down_ref, up_ref, gain_ref, shift_ref, mix_ref, out_ref, fine, sem
):
    members, slots, columns, levels, features = out_ref.shape
    half_rows, inner = slots // 2 + 1, columns - 2
    count = normed_ref.shape[0]
    step = half_rows // count
    pairs = fine.reshape(members, half_rows, 2, inner // 2, 2, levels, features)
    sums = group_sums(2 * features, features)

    def chunk(index, carry):
        down = jnp.concatenate([down_ref[k, PAD : PAD + features] for k in range(4)], axis=0)
        coarse = jnp.dot(normed_ref[index], down, preferred_element_type=F32).astype(BF16)
        for p in range(2):
            grown = jnp.dot(coarse, up_ref[p], preferred_element_type=F32)
            pair = mixed_pair(grown, sums, gain_ref, shift_ref, mix_ref, features)
            for q, mixed in enumerate(pair):
                mixed = mixed.reshape(members, step, inner // 2, levels, features)
                pairs[:, pl.ds(index * step, step), p, :, q] = mixed.astype(BF16)
        return carry

    lax.fori_loop(0, count, chunk, 0)
    odd = cleared(band_ref, fine)
    store = pltpu.make_async_copy(
        fine.at[:, pl.ds(odd, slots)], out_ref.at[:, :, pl.ds(1, inner)], sem
    )
    store.start()
    store.wait()


def inner_of(band_rows, normed, down, up, gain, shift, mix, shape):
    members, slots, columns, levels, features = shape
    return pl.pallas_call(
        inner_kernel,
        out_shape=jax.ShapeDtypeStruct(shape, BF16),
        in_specs=[SMEM] + [VMEM] * 6,
        out_specs=ANY,
        scratch_shapes=[
            pltpu.VMEM((members, slots + 2, columns - 2, levels, features), BF16),
            pltpu.SemaphoreType.DMA,
        ],
        cost_estimate=cost(4 * 10**9, 10**6),
        compiler_params=room(16),
        name="inner",
    )(band_rows, normed, down, up, gain, shift, mix)


def member_means(values, lower, count):
    middle = values[:, LANES : 2 * LANES]
    zero = jnp.zeros_like(middle)
    first = values[:, :LANES] + jnp.where(lower, middle, zero)
    second = values[:, 2 * LANES :] + jnp.where(lower, zero, middle)
    return [
        jnp.broadcast_to(jnp.sum(half, axis=-1, keepdims=True) / count, middle.shape)
        for half in (first, second)
    ]


def outer_kernel(
    band_ref,
    from_west_ref,
    west_ref,
    east_ref,
    from_east_ref,
    gain_ref,
    shift_ref,
    down_ref,
    up_ref,
    up_gain_ref,
    up_shift_ref,
    mix_ref,
    partial_ref,
    out_ref,
    fine,
    sem,
):
    del partial_ref
    members, slots, columns, levels, features = out_ref.shape
    half_rows = slots // 2 + 1
    odd, _ = band(band_ref)
    copies = []
    width = members * features
    lane = lax.broadcasted_iota(jnp.int32, (half_rows * levels, LANES), 1)
    lower = lane < features - LANES
    sums = group_sums(width, features)
    for side, refs in enumerate(((from_west_ref, west_ref), (east_ref, from_east_ref))):
        parts = [
            refs[q].reshape(half_rows, 2, levels, width)[:, p].astype(F32).reshape(-1, width)
            for q, p in ORDER
        ]
        averages = member_means(parts[0] + parts[1] + parts[2] + parts[3], lower, 4 * features)
        average = blended(*averages, features - LANES)
        parts = [part - average for part in parts]
        squares = parts[0] * parts[0]
        for part in parts[1:]:
            squares = squares + part * part
        spreads = member_means(squares, lower, 4 * features)
        scale = blended(*(lax.rsqrt(spread + EPS) for spread in spreads), features - LANES)
        coarse = [None] * members
        for k, part in enumerate(parts):
            normed = (part * scale * gain_ref[k] + shift_ref[k]).astype(BF16)
            for member in range(members):
                term = padded_dot(window(normed, member), down_ref.at[k], member)
                coarse[member] = term if coarse[member] is None else coarse[member] + term
        coarse = jnp.concatenate(coarse, axis=0).astype(BF16)
        q = 1 - side
        lanes = slice(q * LANES, q * LANES + 2 * LANES)
        for p in range(2):
            grown = jnp.dot(coarse, up_ref[p, :, lanes], preferred_element_type=F32)
            squares = (grown * grown).astype(BF16)
            spread = jnp.dot(squares, sums[lanes, q * LANES : (q + 1) * LANES], preferred_element_type=F32)
            scale = lax.rsqrt(spread * (1.0 / features) + EPS)
            scale = jnp.concatenate([scale, scale], axis=-1)
            normed = grown * scale * up_gain_ref[:, lanes] + up_shift_ref[:, lanes]
            mixed = padded_dot(normed.astype(BF16), mix_ref, q)
            mixed = mixed.reshape(members, half_rows, levels, features)
            view = fine.at[side].reshape(members, half_rows, 2, levels, features)
            view[:, :, p] = mixed.astype(BF16)
        cleared(band_ref, fine.at[side])
        copy = pltpu.make_async_copy(
            fine.at[side, :, pl.ds(odd, slots)],
            out_ref.at[:, :, side * (columns - 1)],
            sem.at[side],
        )
        copy.start()
        copies.append(copy)
    for copy in copies:
        copy.wait()


def outer_of(band_rows, sides, gain, shift, down, up, up_gain, up_shift, mix, partial):
    members, slots, columns, levels, features = partial.shape
    return pl.pallas_call(
        outer_kernel,
        out_shape=jax.ShapeDtypeStruct(partial.shape, BF16),
        in_specs=[SMEM] + [VMEM] * 11 + [ANY],
        out_specs=ANY,
        scratch_shapes=[
            pltpu.VMEM((2, members, slots + 2, levels, features), BF16),
            pltpu.SemaphoreType.DMA((2,)),
        ],
        input_output_aliases={12: 0},
        cost_estimate=cost(3 * 10**9, 10**6),
        compiler_params=room(12),
        name="outer",
    )(band_rows, *sides, gain, shift, down, up, up_gain, up_shift, mix, partial)


def assemble_kernel(*refs):
    pieces, (down_ref, up_ref) = refs[:-2], refs[-2:]
    pad = PAD // 8
    lon, lat, up_tiles = up_ref.shape[1:4]
    own = pieces[0]
    tiles = own.shape[0] - 2 * up_tiles
    zero = jnp.zeros((pad,) + own.shape[1:], BF16)
    for part in range(down_ref.shape[0]):
        down_ref[part, :pad] = zero
        down_ref[part, pad + lat * tiles :] = zero
    here, place = lax.axis_index("lon"), lax.axis_index("lat")
    own, z1, z2, z3, core, across, across12, across3, rest, last = pieces
    far = lat - 1 - place
    beside = lax.bitwise_xor(place, 1)
    beside_far = lat - 1 - beside
    n = tiles + 2 * up_tiles
    table = [
        (own, 0, 0, place),
        (z1, 0, 1, place),
        (z2, 0, 2, place),
        (z3, 0, 3, place),
        (core, 0, 0, beside),
        (across, 0, 0, far),
        (across12, 0, 1, far),
        (across12, n, 2, far),
        (across3, 0, 3, far),
        (rest, 0, 1, beside),
        (rest, n, 2, beside),
        (rest, 2 * n, 3, beside),
        (rest, 3 * n, 0, beside_far),
        (rest, 4 * n, 1, beside_far),
        (rest, 5 * n, 2, beside_far),
        (last, 0, 3, beside_far),
    ]
    for ref, at, hop, row in table:
        source = lax.bitwise_xor(here, hop)
        down_ref[source, pl.ds(pad + row * tiles, tiles)] = ref[at : at + tiles]
        up_ref[0, source, row] = ref[at + tiles : at + tiles + up_tiles]
        up_ref[1, source, row] = ref[at + tiles + up_tiles : at + n]


def fast_weights(down, up, first, last, features):
    lon, lat = lax.axis_size("lon"), lax.axis_size("lat")
    tiles, up_tiles = down.shape[0] // 8, up.shape[0] // 8
    place = lax.axis_index("lat")
    with jax.named_scope("shard"):
        shard = shard_of(down, up, features)
    mirror = lambda i: lat - 1 - i
    with jax.named_scope("z2"):
        z2 = swapped(shard, "lon", lambda i: i ^ 2)
    with jax.named_scope("z3"):
        z3 = swapped(shard, "lon", lambda i: i ^ 3)
    with jax.named_scope("z1"):
        z1 = swapped(shard, "lon", lambda i: i ^ 1)
    even = place % 2 == 0
    with jax.named_scope("core"):
        rows = jnp.where(even, last, first)
        core = swapped(jnp.concatenate([shard, rows]), "lat", lambda i: i ^ 1)
    with jax.named_scope("x"):
        rows = jnp.where(even, first, last)
        across = swapped(jnp.concatenate([shard, rows]), "lat", mirror)
    n = shard.shape[0]
    core_rows, across_rows = core[n:], across[n:]
    below = jnp.where(even, core_rows, across_rows)
    below = jnp.where(place == lat - 1, jnp.zeros_like(below), below)
    above = jnp.where(even, across_rows, core_rows)
    with jax.named_scope("x12"):
        across12 = swapped(jnp.concatenate([z1, z2]), "lat", mirror)
    with jax.named_scope("x3"):
        across3 = swapped(z3, "lat", mirror)
    with jax.named_scope("rest"):
        rest = jnp.concatenate([z1, z2, z3, across[:n], across12])
        rest = swapped(rest, "lat", lambda i: i ^ 1)
    with jax.named_scope("last"):
        final = swapped(across3, "lat", lambda i: i ^ 1)
    down, up = pl.pallas_call(
        assemble_kernel,
        out_shape=(
            jax.ShapeDtypeStruct((lon, lat * tiles + PAD // 4, 8, down.shape[1]), BF16),
            jax.ShapeDtypeStruct((2, lon, lat, up_tiles, 8, down.shape[1]), BF16),
        ),
        in_specs=[VMEM] * 10,
        out_specs=(VMEM,) * 2,
        compiler_params=room(6),
        name="assemble",
    )(shard, z1, z2, z3, core, across, across12, across3, rest, final)
    down = down.reshape(4, -1, down.shape[-1])
    return down, up, above, below


def plain_weights(down, up, first, last, features):
    up = centred(up, features)
    below = passed_along(first, "lat", -1)
    above = passed_along(last, "lat", 1)
    rows, half = up.shape[0], up.shape[1] // 2
    shard = jnp.concatenate([down, up[:, :half], up[:, half:]], axis=0)
    whole = lax.all_gather(shard, ("lon", "lat"), axis=0)
    n = down.shape[0]
    up = jnp.stack([whole[:, n : n + rows], whole[:, n + rows :]])
    down = whole[:, :n].reshape(4, features, half)
    return jnp.pad(down, ((0, 0), (PAD, PAD), (0, 0))), up, above, below


def body(
    tokens, band_rows, down_gain, down_shift, down_weight, up_weight, up_gain, up_shift, mix_weight
):
    members, levels, slots, columns, features = tokens.shape
    lon, lat = lax.axis_size("lon"), lax.axis_size("lat")
    block = tokens.transpose(0, 2, 3, 1, 4)
    with jax.named_scope("edges"):
        first, last, west, east = edges_of(band_rows, block)
    plain = lon != 4 or lat != 4 or down_weight.shape[0] % 8 or up_weight.shape[0] % 8
    weights = plain_weights if plain else fast_weights
    down, up, above, below = weights(down_weight, up_weight, first, last, features)
    narrow = down_weight.shape[1]
    up = up.reshape(2, narrow, narrow)
    with jax.named_scope("corners"):
        west, east = with_corners(band_rows, above, below, west, east)
    with jax.named_scope("from_east"):
        from_east = shifted(west, "lon", -1)
    with jax.named_scope("from_west"):
        from_west = shifted(east, "lon", 1)
    gain, shift = down_gain.reshape(4, 1, features), down_shift.reshape(4, 1, features)
    twice = lambda value: jnp.concatenate([value, value], axis=-1)
    fine_gain, fine_shift = twice(up_gain)[None], twice(up_shift)[None]
    mix_weight = jnp.pad(mix_weight, ((PAD, PAD), (0, 0)))
    with jax.named_scope("inner_norm"):
        normed = inner_norm(band_rows, block, above, below, gain, shift)
    with jax.named_scope("inner"):
        out = inner_of(
            band_rows, normed, down, up, fine_gain, fine_shift, mix_weight, block.shape
        )
    with jax.named_scope("outer"):
        out = outer_of(
            band_rows,
            (from_west, west, east, from_east),
            twice(gain),
            twice(shift),
            down,
            up,
            fine_gain,
            fine_shift,
            mix_weight,
            out,
        )
    return out.transpose(0, 3, 1, 2, 4)


def solution(mesh):
    return jax.shard_map(
        body,
        mesh=mesh,
        in_specs=(
            P("mem", None, "lat", "lon", None),
            P("lat", None),
            P(),
            P(),
            P(("lon", "lat"), None),
            P(("lon", "lat"), None),
            P(),
            P(),
            P(),
        ),
        out_specs=P("mem", None, "lat", "lon", None),
        check_vma=False,
    )
```

```python
import jax
import jax.numpy as jnp
from jax import lax
from jax.experimental import pallas as pl
from jax.experimental.pallas import tpu as pltpu
from jax.sharding import PartitionSpec as P


EPS = 1e-05
LANES = 128
PAD = 64
F32 = jnp.float32
BF16 = jnp.bfloat16
VMEM = pl.BlockSpec(memory_space=pltpu.VMEM)
SMEM = pl.BlockSpec(memory_space=pltpu.SMEM)
HBM = pl.BlockSpec(memory_space=pltpu.HBM)
ORDER = ((0, 0), (0, 1), (1, 0), (1, 1))


def passed_along(block, axis, distance):
    devices = range(lax.axis_size(axis))
    route = [(i, i + distance) for i in devices if i + distance in devices]
    return lax.ppermute(block, axis, route)


def swapped(block, axis, partner):
    n = lax.axis_size(axis)
    return lax.ppermute(block, axis, [(i, partner(i)) for i in range(n)])


def band(band_ref):
    odd = lax.rem(band_ref[0, 0], 2)
    return odd, band_ref[0, 1] - band_ref[0, 0]


def room(mebibytes):
    return pltpu.CompilerParams(vmem_limit_bytes=mebibytes * 2**20)


def cost(flops, moved):
    return pl.CostEstimate(flops=flops, bytes_accessed=moved, transcendentals=0)


def centred(weight, features):
    blocks = []
    for start in range(0, weight.shape[-1], features):
        block = weight[..., start : start + features].astype(F32)
        blocks.append(block - jnp.mean(block, axis=-1, keepdims=True))
    return jnp.concatenate(blocks, axis=-1).astype(BF16)


def joined(pair):
    return jnp.concatenate([pair[0].astype(F32), pair[1].astype(F32)], axis=-1).astype(BF16)


def first_kernel(
    band_ref, tokens_ref, down_ref, up_ref, shard_ref, core_ref, across_ref, down_s, up_s, rows, sem
):
    tiles, up_tiles = down_ref.shape[0], up_ref.shape[0]
    half, features = up_ref.shape[2] // 2, tokens_ref.shape[4]
    _, live = band(band_ref)
    even = lax.rem(lax.axis_index("lat"), 2) == 0
    last = live - 1
    sources = [
        (down_ref, down_s),
        (up_ref, up_s),
        (tokens_ref.at[:, jnp.where(even, last, 0)], rows.at[0]),
        (tokens_ref.at[:, jnp.where(even, 0, last)], rows.at[1]),
    ]
    copies = [pltpu.make_async_copy(*pair, sem.at[i]) for i, pair in enumerate(sources)]
    for copy in copies:
        copy.start()
    copies[0].wait()
    copies[1].wait()
    up = centred(up_s[...], features)
    for ref in (shard_ref, core_ref, across_ref):
        ref[:tiles] = down_s[...]
        ref[tiles : tiles + up_tiles] = up[..., :half]
        ref[tiles + up_tiles : tiles + 2 * up_tiles] = up[..., half:]
    for side, ref in enumerate((core_ref, across_ref)):
        copies[2 + side].wait()
        ref[tiles + 2 * up_tiles :] = joined(rows[side])


def first_sends(band_rows, tokens, down, up):
    members, _, columns, levels, features = tokens.shape
    tiles, up_tiles = down.shape[0] // 8, up.shape[0] // 8
    n, wide = tiles + 2 * up_tiles, down.shape[1]
    shard = jax.ShapeDtypeStruct((n, 8, wide), BF16)
    with_row = jax.ShapeDtypeStruct((n + columns, 8, wide), BF16)
    return pl.pallas_call(
        first_kernel,
        out_shape=(shard, with_row, with_row),
        in_specs=[SMEM, HBM, HBM, HBM],
        out_specs=(VMEM,) * 3,
        scratch_shapes=[
            pltpu.VMEM((tiles, 8, wide), BF16),
            pltpu.VMEM((up_tiles, 8, up.shape[1]), BF16),
            pltpu.VMEM((2, members, columns, levels, features), BF16),
            pltpu.SemaphoreType.DMA((4,)),
        ],
        compiler_params=room(2),
        name="first",
    )(band_rows, tokens, down.reshape(tiles, 8, -1), up.reshape(up_tiles, 8, -1))


def rows_kernel(band_ref, tokens_ref, first_ref, last_ref, rows, sem):
    _, live = band(band_ref)
    copies = [
        pltpu.make_async_copy(tokens_ref.at[:, row], rows.at[i], sem.at[i])
        for i, row in enumerate((0, live - 1))
    ]
    for copy in copies:
        copy.start()
    for side, out_ref in enumerate((first_ref, last_ref)):
        copies[side].wait()
        out_ref[...] = joined(rows[side])


def rows_of(band_rows, tokens):
    members, _, columns, levels, features = tokens.shape
    row = jax.ShapeDtypeStruct((columns, levels, members * features), BF16)
    return pl.pallas_call(
        rows_kernel,
        out_shape=(row, row),
        in_specs=[SMEM, HBM],
        out_specs=(VMEM,) * 2,
        scratch_shapes=[
            pltpu.VMEM((2, members, columns, levels, features), BF16),
            pltpu.SemaphoreType.DMA((2,)),
        ],
        compiler_params=room(2),
        name="rows",
    )(band_rows, tokens)


def edges_kernel(band_ref, tokens_ref, west_ref, east_ref, cols, sem):
    slots, columns = tokens_ref.shape[1:3]
    odd, _ = band(band_ref)
    copies = [
        pltpu.make_async_copy(tokens_ref.at[:, :, column], cols.at[i], sem.at[i])
        for i, column in enumerate((0, columns - 1))
    ]
    for copy in copies:
        copy.start()
    for side, out_ref in enumerate((west_ref, east_ref)):
        copies[side].wait()
        out_ref[pl.ds(odd, slots)] = joined(cols[side])


def edges_of(band_rows, tokens):
    members, slots, _, levels, features = tokens.shape
    col = jax.ShapeDtypeStruct((slots + 2, levels, members * features), BF16)
    return pl.pallas_call(
        edges_kernel,
        out_shape=(col, col),
        in_specs=[SMEM, HBM],
        out_specs=(VMEM,) * 2,
        scratch_shapes=[
            pltpu.VMEM((2, members, slots, levels, features), BF16),
            pltpu.SemaphoreType.DMA((2,)),
        ],
        compiler_params=room(2),
        name="edges",
    )(band_rows, tokens)


def corners_kernel(band_ref, above_ref, below_ref, west_in, east_in, *out_refs):
    odd, live = band(band_ref)
    columns = above_ref.shape[0]
    west_ref, east_ref, near_ref, far_ref = out_refs
    west_ref[...] = west_in[...]
    east_ref[...] = east_in[...]
    for column, out_ref in ((0, west_ref), (columns - 1, east_ref)):
        out_ref[pl.ds(live + odd, 1)] = below_ref[pl.ds(column, 1)]

        @pl.when(odd == 1)
        def _():
            out_ref[pl.ds(0, 1)] = above_ref[pl.ds(column, 1)]

    even = lax.rem(lax.axis_index("lon"), 2) == 0

    @pl.when(even)
    def _():
        near_ref[...] = east_ref[...]
        far_ref[...] = west_ref[...]

    @pl.when(jnp.logical_not(even))
    def _():
        near_ref[...] = west_ref[...]
        far_ref[...] = east_ref[...]


def with_corners(band_rows, above, below, west, east):
    out = jax.ShapeDtypeStruct(west.shape, BF16)
    return pl.pallas_call(
        corners_kernel,
        out_shape=(out,) * 4,
        in_specs=[SMEM] + [VMEM] * 4,
        out_specs=(VMEM,) * 4,
        compiler_params=room(1),
        name="corners",
    )(band_rows, above, below, west, east)


def stacked(pieces, lengths):
    def kernel(*refs):
        start = 0
        for ref, length in zip(refs[:-1], lengths):
            refs[-1][start : start + length] = ref[:length]
            start += length

    return pl.pallas_call(
        kernel,
        out_shape=jax.ShapeDtypeStruct((sum(lengths),) + pieces[0].shape[1:], BF16),
        in_specs=[VMEM] * len(pieces),
        out_specs=VMEM,
        compiler_params=room(1),
        name="stacked",
    )(*pieces)


def merge_normed(parts, gain_ref, shift_ref):
    features = parts[0].shape[-1]
    total = parts[0] + parts[1] + parts[2] + parts[3]
    average = jnp.sum(total, axis=-1, keepdims=True) / (4 * features)
    parts = [part - average for part in parts]
    squares = parts[0] * parts[0]
    for part in parts[1:]:
        squares = squares + part * part
    spread = jnp.sum(squares, axis=-1, keepdims=True) / (4 * features)
    scale = lax.rsqrt(spread + EPS)
    return [
        (part * scale * gain_ref[k] + shift_ref[k]).astype(BF16) for k, part in enumerate(parts)
    ]


def group_sums(width, features):
    shape = (width, 2 * LANES)
    first = lax.broadcasted_iota(jnp.int32, shape, 0) < features
    low = lax.broadcasted_iota(jnp.int32, shape, 1) < LANES
    return jnp.where(first == low, 1.0, 0.0).astype(BF16)


def blended(low, high, rest):
    lane = lax.broadcasted_iota(jnp.int32, low.shape, 1)
    return jnp.concatenate([low, jnp.where(lane < rest, low, high), high], axis=-1)


def window(rows, q):
    return rows[:, q * LANES : q * LANES + 2 * LANES]


def mixed_pair(grown, sums, gain_ref, shift_ref, mix_ref, features):
    squares = (grown * grown).astype(BF16)
    spread = jnp.dot(squares, sums, preferred_element_type=F32)
    scale = lax.rsqrt(spread * (1.0 / features) + EPS)
    scale = blended(scale[:, :LANES], scale[:, LANES:], features - LANES)
    normed = (grown * scale * gain_ref[...] + shift_ref[...]).astype(BF16)
    return [padded_dot(window(normed, q), mix_ref, q) for q in range(2)]


def padded_dot(rows, weight_ref, q):
    start = (1 - q) * PAD
    weight = weight_ref[start : start + 2 * LANES]
    return jnp.dot(rows, weight, preferred_element_type=F32)


def cleared(band_ref, fine):
    odd, live = band(band_ref)
    members, rows = fine.shape[:2]

    def clear(row, carry):
        fine[:, pl.ds(row, 1)] = jnp.zeros((members, 1) + fine.shape[2:], BF16)
        return carry

    lax.fori_loop(live + odd, rows, clear, 0)
    return odd


def inner_norm_kernel(
    band_ref, tokens_ref, above_ref, below_ref, gain_ref, shift_ref, out_ref, field, sem
):
    members, slots, columns, levels, features = tokens_ref.shape
    half_rows, inner = slots // 2 + 1, columns - 2
    odd, live = band(band_ref)
    load = pltpu.make_async_copy(
        tokens_ref.at[:, :, pl.ds(1, inner)], field.at[:, pl.ds(odd, slots)], sem
    )
    load.start()
    load.wait()
    for member in range(members):
        lanes = slice(member * features, (member + 1) * features)

        @pl.when(odd == 1)
        def _():
            row = above_ref[1 : columns - 1].astype(F32)[..., lanes]
            field[member, pl.ds(0, 1)] = row.astype(BF16)[None]

        row = below_ref[1 : columns - 1].astype(F32)[..., lanes]
        field[member, pl.ds(live + odd, 1)] = row.astype(BF16)[None]
    pairs = field.reshape(members, half_rows, 2, inner // 2, 2, levels, features)
    step = out_ref.shape[1] // (members * inner // 2 * levels)

    def chunk(index, carry):
        parts = [
            pairs[:, pl.ds(index * step, step), p, :, q].astype(F32).reshape(-1, features)
            for q, p in ORDER
        ]
        out_ref[index] = jnp.concatenate(merge_normed(parts, gain_ref, shift_ref), axis=-1)
        return carry

    lax.fori_loop(0, out_ref.shape[0], chunk, 0)


def steps_of(half_rows):
    return max(step for step in range(1, 7) if half_rows % step == 0)


def inner_norm(band_rows, tokens, above, below, gain, shift):
    members, slots, columns, levels, features = tokens.shape
    half_rows, inner = slots // 2 + 1, columns - 2
    step = steps_of(half_rows)
    rows = step * members * inner // 2 * levels
    return pl.pallas_call(
        inner_norm_kernel,
        out_shape=jax.ShapeDtypeStruct((half_rows // step, rows, 4 * features), BF16),
        in_specs=[SMEM, HBM] + [VMEM] * 4,
        out_specs=VMEM,
        scratch_shapes=[
            pltpu.VMEM((members, slots + 2, inner, levels, features), BF16),
            pltpu.SemaphoreType.DMA,
        ],
        cost_estimate=cost(10**9, 10**6),
        compiler_params=room(10),
        name="inner_norm",
    )(band_rows, tokens, above, below, gain, shift)


def inner_kernel(
    band_ref, normed_ref, down_ref, up_ref, gain_ref, shift_ref, mix_ref, out_ref, fine, sem
):
    members, slots, columns, levels, features = out_ref.shape
    half_rows, inner = slots // 2 + 1, columns - 2
    count = normed_ref.shape[0]
    step = half_rows // count
    pairs = fine.reshape(members, half_rows, 2, inner // 2, 2, levels, features)
    sums = group_sums(2 * features, features)

    def chunk(index, carry):
        down = jnp.concatenate([down_ref[k, PAD : PAD + features] for k in range(4)], axis=0)
        coarse = jnp.dot(normed_ref[index], down, preferred_element_type=F32).astype(BF16)
        for p in range(2):
            grown = jnp.dot(coarse, up_ref[p], preferred_element_type=F32)
            pair = mixed_pair(grown, sums, gain_ref, shift_ref, mix_ref, features)
            for q, mixed in enumerate(pair):
                mixed = mixed.reshape(members, step, inner // 2, levels, features)
                pairs[:, pl.ds(index * step, step), p, :, q] = mixed.astype(BF16)
        return carry

    lax.fori_loop(0, count, chunk, 0)
    odd = cleared(band_ref, fine)
    store = pltpu.make_async_copy(
        fine.at[:, pl.ds(odd, slots)], out_ref.at[:, :, pl.ds(1, inner)], sem
    )
    store.start()
    store.wait()


def inner_of(band_rows, normed, down, up, gain, shift, mix, shape):
    members, slots, columns, levels, features = shape
    return pl.pallas_call(
        inner_kernel,
        out_shape=jax.ShapeDtypeStruct(shape, BF16),
        in_specs=[SMEM] + [VMEM] * 6,
        out_specs=HBM,
        scratch_shapes=[
            pltpu.VMEM((members, slots + 2, columns - 2, levels, features), BF16),
            pltpu.SemaphoreType.DMA,
        ],
        cost_estimate=cost(4 * 10**9, 10**6),
        compiler_params=room(16),
        name="inner",
    )(band_rows, normed, down, up, gain, shift, mix)


def rows_at(ref, p):
    rows, levels, width = ref.shape
    half = ref.reshape(rows // 2, 2, levels, width)[:, p]
    return half.astype(F32).reshape(-1, width)


def member_means(values, lower, count):
    middle = values[:, LANES : 2 * LANES]
    zero = jnp.zeros_like(middle)
    first = values[:, :LANES] + jnp.where(lower, middle, zero)
    second = values[:, 2 * LANES :] + jnp.where(lower, zero, middle)
    return [
        jnp.broadcast_to(jnp.sum(half, axis=-1, keepdims=True) / count, middle.shape)
        for half in (first, second)
    ]


def outer_kernel(
    band_ref,
    near_ref,
    west_ref,
    east_ref,
    far_ref,
    gain_ref,
    shift_ref,
    down_ref,
    up_ref,
    up_gain_ref,
    up_shift_ref,
    mix_ref,
    partial_ref,
    out_ref,
    fine,
    sem,
):
    del partial_ref
    members, slots, columns, levels, features = out_ref.shape
    half_rows = slots // 2 + 1
    odd, _ = band(band_ref)
    copies = []
    width = members * features
    lane = lax.broadcasted_iota(jnp.int32, (half_rows * levels, LANES), 1)
    lower = lane < features - LANES
    sums = group_sums(width, features)
    even = lax.rem(lax.axis_index("lon"), 2) == 0
    for side in range(2):
        parts = []
        for q, p in ORDER:
            ref = (west_ref, east_ref)[side] if q != side else None
            if ref is not None:
                part = rows_at(ref, p)
            else:
                part = jnp.where(even == (side == 0), rows_at(far_ref, p), rows_at(near_ref, p))
            parts.append(part)
        averages = member_means(parts[0] + parts[1] + parts[2] + parts[3], lower, 4 * features)
        average = blended(*averages, features - LANES)
        parts = [part - average for part in parts]
        squares = parts[0] * parts[0]
        for part in parts[1:]:
            squares = squares + part * part
        spreads = member_means(squares, lower, 4 * features)
        scale = blended(*(lax.rsqrt(spread + EPS) for spread in spreads), features - LANES)
        coarse = [None] * members
        for k, part in enumerate(parts):
            normed = (part * scale * gain_ref[k] + shift_ref[k]).astype(BF16)
            for member in range(members):
                term = padded_dot(window(normed, member), down_ref.at[k], member)
                coarse[member] = term if coarse[member] is None else coarse[member] + term
        coarse = jnp.concatenate(coarse, axis=0).astype(BF16)
        q = 1 - side
        lanes = slice(q * LANES, q * LANES + 2 * LANES)
        for p in range(2):
            grown = jnp.dot(coarse, up_ref[p, :, lanes], preferred_element_type=F32)
            squares = (grown * grown).astype(BF16)
            spread = jnp.dot(squares, sums[lanes, q * LANES : (q + 1) * LANES], preferred_element_type=F32)
            scale = lax.rsqrt(spread * (1.0 / features) + EPS)
            scale = jnp.concatenate([scale, scale], axis=-1)
            normed = grown * scale * up_gain_ref[:, lanes] + up_shift_ref[:, lanes]
            mixed = padded_dot(normed.astype(BF16), mix_ref, q)
            mixed = mixed.reshape(members, half_rows, levels, features)
            view = fine.at[side].reshape(members, half_rows, 2, levels, features)
            view[:, :, p] = mixed.astype(BF16)
        cleared(band_ref, fine.at[side])
        copy = pltpu.make_async_copy(
            fine.at[side, :, pl.ds(odd, slots)],
            out_ref.at[:, :, side * (columns - 1)],
            sem.at[side],
        )
        copy.start()
        copies.append(copy)
    for copy in copies:
        copy.wait()


def outer_of(band_rows, sides, gain, shift, down, up, up_gain, up_shift, mix, partial):
    members, slots, _, levels, features = partial.shape
    return pl.pallas_call(
        outer_kernel,
        out_shape=jax.ShapeDtypeStruct(partial.shape, BF16),
        in_specs=[SMEM] + [VMEM] * 11 + [HBM],
        out_specs=HBM,
        scratch_shapes=[
            pltpu.VMEM((2, members, slots + 2, levels, features), BF16),
            pltpu.SemaphoreType.DMA((2,)),
        ],
        input_output_aliases={12: 0},
        cost_estimate=cost(3 * 10**9, 10**6),
        compiler_params=room(12),
        name="outer",
    )(band_rows, *sides, gain, shift, down, up, up_gain, up_shift, mix, partial)


def assemble_kernel(*refs):
    pieces, (down_ref, up_ref) = refs[:-2], refs[-2:]
    pad = PAD // 8
    _, lat, up_tiles = up_ref.shape[1:4]
    own = pieces[0]
    tiles = own.shape[0] - 2 * up_tiles
    zero = jnp.zeros((pad,) + own.shape[1:], BF16)
    for part in range(down_ref.shape[0]):
        down_ref[part, :pad] = zero
        down_ref[part, pad + lat * tiles :] = zero
    here, place = lax.axis_index("lon"), lax.axis_index("lat")
    own, z1, z2, z3, core, across, across12, across3, rest, last = pieces
    far = lat - 1 - place
    beside = lax.bitwise_xor(place, 1)
    beside_far = lat - 1 - beside
    n = tiles + 2 * up_tiles
    table = [
        (own, 0, 0, place),
        (z1, 0, 1, place),
        (z2, 0, 2, place),
        (z3, 0, 3, place),
        (core, 0, 0, beside),
        (across, 0, 0, far),
        (across12, 0, 1, far),
        (across12, n, 2, far),
        (across3, 0, 3, far),
        (rest, 0, 1, beside),
        (rest, n, 2, beside),
        (rest, 2 * n, 3, beside),
        (rest, 3 * n, 0, beside_far),
        (rest, 4 * n, 1, beside_far),
        (rest, 5 * n, 2, beside_far),
        (last, 0, 3, beside_far),
    ]
    for ref, at, hop, row in table:
        source = lax.bitwise_xor(here, hop)
        down_ref[source, pl.ds(pad + row * tiles, tiles)] = ref[at : at + tiles]
        up_ref[0, source, row] = ref[at + tiles : at + tiles + up_tiles]
        up_ref[1, source, row] = ref[at + tiles + up_tiles : at + n]


def fast_weights(band_rows, tokens, down, up, features):
    lon, lat = lax.axis_size("lon"), lax.axis_size("lat")
    tiles, up_tiles = down.shape[0] // 8, up.shape[0] // 8
    place = lax.axis_index("lat")
    beside, mirror = lambda i: i ^ 1, lambda i: lat - 1 - i
    shard, core, across = first_sends(band_rows, tokens, down, up)
    core = swapped(core, "lat", beside)
    across = swapped(across, "lat", mirror)
    z2 = swapped(shard, "lon", lambda i: i ^ 2)
    z3 = swapped(shard, "lon", lambda i: i ^ 3)
    z1 = swapped(shard, "lon", beside)
    even = place % 2 == 0
    n = shard.shape[0]
    core_rows, across_rows = core[n:], across[n:]
    below = jnp.where(even, core_rows, across_rows)
    below = jnp.where(place == lat - 1, jnp.zeros_like(below), below)
    above = jnp.where(even, across_rows, core_rows)
    across12 = swapped(jnp.concatenate([z1, z2]), "lat", mirror)
    across3 = swapped(z3, "lat", mirror)
    rest = stacked([z1, z2, z3, across, across12], [n, n, n, n, 2 * n])
    rest = swapped(rest, "lat", beside)
    final = swapped(across3, "lat", beside)
    down, up = pl.pallas_call(
        assemble_kernel,
        out_shape=(
            jax.ShapeDtypeStruct((lon, lat * tiles + PAD // 4, 8, down.shape[1]), BF16),
            jax.ShapeDtypeStruct((2, lon, lat, up_tiles, 8, down.shape[1]), BF16),
        ),
        in_specs=[VMEM] * 10,
        out_specs=(VMEM,) * 2,
        compiler_params=room(6),
        name="assemble",
    )(shard, z1, z2, z3, core, across, across12, across3, rest, final)
    down = down.reshape(4, -1, down.shape[-1])
    return down, up, above, below


def plain_weights(band_rows, tokens, down, up, features):
    first, last = rows_of(band_rows, tokens)
    up = centred(up, features)
    below = passed_along(first, "lat", -1)
    above = passed_along(last, "lat", 1)
    rows, half = up.shape[0], up.shape[1] // 2
    shard = jnp.concatenate([down, up[:, :half], up[:, half:]], axis=0)
    whole = lax.all_gather(shard, ("lon", "lat"), axis=0)
    n = down.shape[0]
    up = jnp.stack([whole[:, n : n + rows], whole[:, n + rows :]])
    down = whole[:, :n].reshape(4, features, half)
    return jnp.pad(down, ((0, 0), (PAD, PAD), (0, 0))), up, above, below


def whole(
    tokens, band_rows, down_gain, down_shift, down_weight, up_weight, up_gain, up_shift, mix_weight
):
    _, _, _, _, features = tokens.shape
    lon, lat = lax.axis_size("lon"), lax.axis_size("lat")
    block = tokens.transpose(0, 2, 3, 1, 4)
    west, east = edges_of(band_rows, block)
    plain = lon != 4 or lat != 4 or down_weight.shape[0] % 8 or up_weight.shape[0] % 8
    weights = plain_weights if plain else fast_weights
    down, up, above, below = weights(band_rows, block, down_weight, up_weight, features)
    narrow = down_weight.shape[1]
    up = up.reshape(2, narrow, narrow)
    west, east, near, far = with_corners(band_rows, above, below, west, east)
    far = swapped(far, "lon", lambda i: (i - 1 if i % 2 == 0 else i + 1) % lon)
    near = swapped(near, "lon", lambda i: i ^ 1)
    gain, shift = down_gain.reshape(4, 1, features), down_shift.reshape(4, 1, features)
    twice = lambda value: jnp.concatenate([value, value], axis=-1)
    fine_gain, fine_shift = twice(up_gain)[None], twice(up_shift)[None]
    mix_weight = jnp.pad(mix_weight, ((PAD, PAD), (0, 0)))
    normed = inner_norm(band_rows, block, above, below, gain, shift)
    out = inner_of(
        band_rows, normed, down, up, fine_gain, fine_shift, mix_weight, block.shape
    )
    out = outer_of(
        band_rows,
        (near, west, east, far),
        twice(gain),
        twice(shift),
        down,
        up,
        fine_gain,
        fine_shift,
        mix_weight,
        out,
    )
    return out.transpose(0, 3, 1, 2, 4)


def solution(mesh):
    return jax.shard_map(
        whole,
        mesh=mesh,
        in_specs=(
            P("mem", None, "lat", "lon", None),
            P("lat", None),
            P(),
            P(),
            P(("lon", "lat"), None),
            P(("lon", "lat"), None),
            P(),
            P(),
            P(),
        ),
        out_specs=P("mem", None, "lat", "lon", None),
        check_vma=False,
    )
```

```python
import jax
import jax.numpy as jnp
from jax import lax
from jax.experimental import pallas as pl
from jax.experimental.pallas import tpu as pltpu
from jax.sharding import PartitionSpec as P


EPS = 1e-05
LANES = 128
PAD = 64
F32 = jnp.float32
BF16 = jnp.bfloat16
VMEM = pl.BlockSpec(memory_space=pltpu.VMEM)
SMEM = pl.BlockSpec(memory_space=pltpu.SMEM)
HBM = pl.BlockSpec(memory_space=pltpu.HBM)
ORDER = ((0, 0), (0, 1), (1, 0), (1, 1))


def passed_along(block, axis, distance):
    devices = range(lax.axis_size(axis))
    route = [(i, i + distance) for i in devices if i + distance in devices]
    return lax.ppermute(block, axis, route)


def swapped(block, axis, partner):
    n = lax.axis_size(axis)
    return lax.ppermute(block, axis, [(i, partner(i)) for i in range(n)])


def band(band_ref):
    odd = lax.rem(band_ref[0, 0], 2)
    return odd, band_ref[0, 1] - band_ref[0, 0]


def room(mebibytes):
    return pltpu.CompilerParams(vmem_limit_bytes=mebibytes * 2**20)


def cost(flops, moved):
    return pl.CostEstimate(flops=flops, bytes_accessed=moved, transcendentals=0)


def centred(weight, features):
    blocks = []
    for start in range(0, weight.shape[-1], features):
        block = weight[..., start : start + features].astype(F32)
        blocks.append(block - jnp.mean(block, axis=-1, keepdims=True))
    return jnp.concatenate(blocks, axis=-1).astype(BF16)


def joined(pair):
    return jnp.concatenate([pair[0].astype(F32), pair[1].astype(F32)], axis=-1).astype(BF16)


def held(array):
    return pltpu.with_memory_space_constraint(array, pltpu.HBM)


def first_kernel(
    band_hbm,
    tokens_ref,
    down_ref,
    up_ref,
    shard_ref,
    core_ref,
    across_ref,
    west_ref,
    east_ref,
    tokens_s,
    band_s,
    down_s,
    up_s,
    sem,
):
    tiles, up_tiles = down_ref.shape[0], up_ref.shape[0]
    slots, columns = tokens_ref.shape[1:3]
    half, features = up_ref.shape[2] // 2, tokens_ref.shape[4]
    sources = [(down_ref, down_s), (up_ref, up_s), (band_hbm, band_s), (tokens_ref, tokens_s)]
    copies = [pltpu.make_async_copy(*pair, sem.at[i]) for i, pair in enumerate(sources)]
    for copy in copies:
        copy.start()
    copies[0].wait()
    copies[1].wait()
    up = centred(up_s[...], features)
    for ref in (shard_ref, core_ref, across_ref):
        ref[:tiles] = down_s[...]
        ref[tiles : tiles + up_tiles] = up[..., :half]
        ref[tiles + up_tiles : tiles + 2 * up_tiles] = up[..., half:]
    copies[2].wait()
    odd, live = band(band_s)
    even = lax.rem(lax.axis_index("lat"), 2) == 0
    last = live - 1
    copies[3].wait()
    for ref, row in ((core_ref, jnp.where(even, last, 0)), (across_ref, jnp.where(even, 0, last))):
        ref[tiles + 2 * up_tiles :] = joined(tokens_s[:, row])
    for ref, column in ((west_ref, 0), (east_ref, columns - 1)):
        ref[pl.ds(odd, slots)] = joined(tokens_s[:, :, column])


def first_sends(band_rows, tokens, down, up):
    members, slots, columns, levels, features = tokens.shape
    tiles, up_tiles = down.shape[0] // 8, up.shape[0] // 8
    n, wide = tiles + 2 * up_tiles, down.shape[1]
    shard = jax.ShapeDtypeStruct((n, 8, wide), BF16)
    with_row = jax.ShapeDtypeStruct((n + columns, 8, wide), BF16)
    col = jax.ShapeDtypeStruct((slots + 2, levels, members * features), BF16)
    return pl.pallas_call(
        first_kernel,
        out_shape=(shard, with_row, with_row, col, col, jax.ShapeDtypeStruct(tokens.shape, BF16)),
        in_specs=[HBM] * 4,
        out_specs=(VMEM,) * 6,
        scratch_shapes=[
            pltpu.SMEM(band_rows.shape, jnp.int32),
            pltpu.VMEM((tiles, 8, wide), BF16),
            pltpu.VMEM((up_tiles, 8, up.shape[1]), BF16),
            pltpu.SemaphoreType.DMA((4,)),
        ],
        compiler_params=room(5),
        name="first",
    )(
        held(band_rows),
        held(tokens),
        held(down.reshape(tiles, 8, -1)),
        held(up.reshape(up_tiles, 8, -1)),
    )


def rows_kernel(band_ref, tokens_ref, first_ref, last_ref, rows, sem):
    _, live = band(band_ref)
    copies = [
        pltpu.make_async_copy(tokens_ref.at[:, row], rows.at[i], sem.at[i])
        for i, row in enumerate((0, live - 1))
    ]
    for copy in copies:
        copy.start()
    for side, out_ref in enumerate((first_ref, last_ref)):
        copies[side].wait()
        out_ref[...] = joined(rows[side])


def rows_of(band_rows, tokens):
    members, _, columns, levels, features = tokens.shape
    row = jax.ShapeDtypeStruct((columns, levels, members * features), BF16)
    return pl.pallas_call(
        rows_kernel,
        out_shape=(row, row),
        in_specs=[SMEM, HBM],
        out_specs=(VMEM,) * 2,
        scratch_shapes=[
            pltpu.VMEM((2, members, columns, levels, features), BF16),
            pltpu.SemaphoreType.DMA((2,)),
        ],
        compiler_params=room(2),
        name="rows",
    )(band_rows, held(tokens))


def edges_kernel(band_ref, tokens_ref, west_ref, east_ref, cols, sem):
    slots, columns = tokens_ref.shape[1:3]
    odd, _ = band(band_ref)
    copies = [
        pltpu.make_async_copy(tokens_ref.at[:, :, column], cols.at[i], sem.at[i])
        for i, column in enumerate((0, columns - 1))
    ]
    for copy in copies:
        copy.start()
    for side, out_ref in enumerate((west_ref, east_ref)):
        copies[side].wait()
        out_ref[pl.ds(odd, slots)] = joined(cols[side])


def edges_of(band_rows, tokens):
    members, slots, _, levels, features = tokens.shape
    col = jax.ShapeDtypeStruct((slots + 2, levels, members * features), BF16)
    return pl.pallas_call(
        edges_kernel,
        out_shape=(col, col),
        in_specs=[SMEM, HBM],
        out_specs=(VMEM,) * 2,
        scratch_shapes=[
            pltpu.VMEM((2, members, slots, levels, features), BF16),
            pltpu.SemaphoreType.DMA((2,)),
        ],
        compiler_params=room(2),
        name="edges",
    )(band_rows, held(tokens))


def corners_kernel(band_ref, above_ref, below_ref, west_ref, east_ref, near_ref, far_ref):
    odd, live = band(band_ref)
    columns = above_ref.shape[0]
    even = lax.rem(lax.axis_index("lon"), 2) == 0
    for mine, refs in ((even, (far_ref, near_ref)), (jnp.logical_not(even), (near_ref, far_ref))):

        @pl.when(mine)
        def _():
            for column, in_ref, out_ref in zip((0, columns - 1), (west_ref, east_ref), refs):
                out_ref[...] = in_ref[...]
                out_ref[pl.ds(live + odd, 1)] = below_ref[pl.ds(column, 1)]

                @pl.when(odd == 1)
                def _():
                    out_ref[pl.ds(0, 1)] = above_ref[pl.ds(column, 1)]


def with_corners(band_rows, above, below, west, east):
    out = jax.ShapeDtypeStruct(west.shape, BF16)
    return pl.pallas_call(
        corners_kernel,
        out_shape=(out, out),
        in_specs=[SMEM] + [VMEM] * 4,
        out_specs=(VMEM,) * 2,
        compiler_params=room(1),
        name="corners",
    )(band_rows, above, below, west, east)


def stacked(pieces, lengths):
    def kernel(*refs):
        start = 0
        for ref, length in zip(refs[:-1], lengths):
            refs[-1][start : start + length] = ref[:length]
            start += length

    return pl.pallas_call(
        kernel,
        out_shape=jax.ShapeDtypeStruct((sum(lengths),) + pieces[0].shape[1:], BF16),
        in_specs=[VMEM] * len(pieces),
        out_specs=VMEM,
        compiler_params=room(1),
        name="stacked",
    )(*pieces)


def merge_normed(parts, gain_ref, shift_ref):
    features = parts[0].shape[-1]
    total = parts[0] + parts[1] + parts[2] + parts[3]
    average = jnp.sum(total, axis=-1, keepdims=True) / (4 * features)
    parts = [part - average for part in parts]
    squares = parts[0] * parts[0]
    for part in parts[1:]:
        squares = squares + part * part
    spread = jnp.sum(squares, axis=-1, keepdims=True) / (4 * features)
    scale = lax.rsqrt(spread + EPS)
    return [
        (part * scale * gain_ref[k] + shift_ref[k]).astype(BF16) for k, part in enumerate(parts)
    ]


def group_sums(width, features):
    shape = (width, 2 * LANES)
    first = lax.broadcasted_iota(jnp.int32, shape, 0) < features
    low = lax.broadcasted_iota(jnp.int32, shape, 1) < LANES
    return jnp.where(first == low, 1.0, 0.0).astype(BF16)


def blended(low, high, rest):
    lane = lax.broadcasted_iota(jnp.int32, low.shape, 1)
    return jnp.concatenate([low, jnp.where(lane < rest, low, high), high], axis=-1)


def window(rows, q):
    return rows[:, q * LANES : q * LANES + 2 * LANES]


def mixed_pair(grown, sums, gain_ref, shift_ref, mix_ref, features):
    squares = (grown * grown).astype(BF16)
    spread = jnp.dot(squares, sums, preferred_element_type=F32)
    scale = lax.rsqrt(spread * (1.0 / features) + EPS)
    scale = blended(scale[:, :LANES], scale[:, LANES:], features - LANES)
    normed = (grown * scale * gain_ref[...] + shift_ref[...]).astype(BF16)
    return [padded_dot(window(normed, q), mix_ref, q) for q in range(2)]


def padded_dot(rows, weight_ref, q):
    start = (1 - q) * PAD
    weight = weight_ref[start : start + 2 * LANES]
    return jnp.dot(rows, weight, preferred_element_type=F32)


def cleared(band_ref, fine):
    odd, live = band(band_ref)
    members, rows = fine.shape[:2]

    def clear(row, carry):
        fine[:, pl.ds(row, 1)] = jnp.zeros((members, 1) + fine.shape[2:], BF16)
        return carry

    lax.fori_loop(live + odd, rows, clear, 0)
    return odd


def inner_norm_kernel(
    band_ref, tokens_ref, above_ref, below_ref, gain_ref, shift_ref, out_ref, field, sem
):
    members, slots, columns, levels, features = tokens_ref.shape
    half_rows, inner = slots // 2 + 1, columns - 2
    odd, live = band(band_ref)
    load = pltpu.make_async_copy(
        tokens_ref.at[:, :, pl.ds(1, inner)], field.at[:, pl.ds(odd, slots)], sem
    )
    load.start()
    load.wait()
    for member in range(members):
        lanes = slice(member * features, (member + 1) * features)

        @pl.when(odd == 1)
        def _():
            row = above_ref[1 : columns - 1].astype(F32)[..., lanes]
            field[member, pl.ds(0, 1)] = row.astype(BF16)[None]

        row = below_ref[1 : columns - 1].astype(F32)[..., lanes]
        field[member, pl.ds(live + odd, 1)] = row.astype(BF16)[None]
    pairs = field.reshape(members, half_rows, 2, inner // 2, 2, levels, features)
    step = out_ref.shape[1] // (members * inner // 2 * levels)

    def chunk(index, carry):
        parts = [
            pairs[:, pl.ds(index * step, step), p, :, q].astype(F32).reshape(-1, features)
            for q, p in ORDER
        ]
        out_ref[index] = jnp.concatenate(merge_normed(parts, gain_ref, shift_ref), axis=-1)
        return carry

    lax.fori_loop(0, out_ref.shape[0], chunk, 0)


def steps_of(half_rows):
    return max(step for step in range(1, 7) if half_rows % step == 0)


def inner_norm(band_rows, tokens, above, below, gain, shift):
    members, slots, columns, levels, features = tokens.shape
    half_rows, inner = slots // 2 + 1, columns - 2
    step = steps_of(half_rows)
    rows = step * members * inner // 2 * levels
    return pl.pallas_call(
        inner_norm_kernel,
        out_shape=jax.ShapeDtypeStruct((half_rows // step, rows, 4 * features), BF16),
        in_specs=[SMEM] + [VMEM] * 5,
        out_specs=VMEM,
        scratch_shapes=[
            pltpu.VMEM((members, slots + 2, inner, levels, features), BF16),
            pltpu.SemaphoreType.DMA,
        ],
        cost_estimate=cost(10**9, 10**6),
        compiler_params=room(10),
        name="inner_norm",
    )(band_rows, tokens, above, below, gain, shift)


def inner_kernel(
    band_ref, normed_ref, down_ref, up_ref, gain_ref, shift_ref, mix_ref, out_ref, fine, sem
):
    members, slots, columns, levels, features = out_ref.shape
    half_rows, inner = slots // 2 + 1, columns - 2
    count = normed_ref.shape[0]
    step = half_rows // count
    pairs = fine.reshape(members, half_rows, 2, inner // 2, 2, levels, features)
    sums = group_sums(2 * features, features)

    def chunk(index, carry):
        down = jnp.concatenate([down_ref[k, PAD : PAD + features] for k in range(4)], axis=0)
        coarse = jnp.dot(normed_ref[index], down, preferred_element_type=F32).astype(BF16)
        for p in range(2):
            grown = jnp.dot(coarse, up_ref[p], preferred_element_type=F32)
            pair = mixed_pair(grown, sums, gain_ref, shift_ref, mix_ref, features)
            for q, mixed in enumerate(pair):
                mixed = mixed.reshape(members, step, inner // 2, levels, features)
                pairs[:, pl.ds(index * step, step), p, :, q] = mixed.astype(BF16)
        return carry

    lax.fori_loop(0, count, chunk, 0)
    odd = cleared(band_ref, fine)
    store = pltpu.make_async_copy(
        fine.at[:, pl.ds(odd, slots)], out_ref.at[:, :, pl.ds(1, inner)], sem
    )
    store.start()
    store.wait()


def inner_of(band_rows, normed, down, up, gain, shift, mix, shape):
    members, slots, columns, levels, features = shape
    return pl.pallas_call(
        inner_kernel,
        out_shape=jax.ShapeDtypeStruct(shape, BF16),
        in_specs=[SMEM] + [VMEM] * 6,
        out_specs=HBM,
        scratch_shapes=[
            pltpu.VMEM((members, slots + 2, columns - 2, levels, features), BF16),
            pltpu.SemaphoreType.DMA,
        ],
        cost_estimate=cost(4 * 10**9, 10**6),
        compiler_params=room(16),
        name="inner",
    )(band_rows, normed, down, up, gain, shift, mix)


def rows_at(ref, p):
    rows, levels, width = ref.shape
    half = ref.reshape(rows // 2, 2, levels, width)[:, p]
    return half.astype(F32).reshape(-1, width)


def member_means(values, lower, count):
    middle = values[:, LANES : 2 * LANES]
    zero = jnp.zeros_like(middle)
    first = values[:, :LANES] + jnp.where(lower, middle, zero)
    second = values[:, 2 * LANES :] + jnp.where(lower, zero, middle)
    return [
        jnp.broadcast_to(jnp.sum(half, axis=-1, keepdims=True) / count, middle.shape)
        for half in (first, second)
    ]


def outer_kernel(
    band_ref,
    near_ref,
    far_ref,
    own_near_ref,
    own_far_ref,
    gain_ref,
    shift_ref,
    down_ref,
    up_ref,
    up_gain_ref,
    up_shift_ref,
    mix_ref,
    partial_ref,
    out_ref,
    fine,
    sem,
):
    del partial_ref
    members, slots, columns, levels, features = out_ref.shape
    half_rows = slots // 2 + 1
    odd, _ = band(band_ref)
    copies = []
    width = members * features
    lane = lax.broadcasted_iota(jnp.int32, (half_rows * levels, LANES), 1)
    lower = lane < features - LANES
    sums = group_sums(width, features)
    even = lax.rem(lax.axis_index("lon"), 2) == 0
    for side in range(2):
        parts = []
        for q, p in ORDER:
            refs = (own_far_ref, own_near_ref) if q != side else (far_ref, near_ref)
            part = jnp.where(even == (side == 0), *(rows_at(ref, p) for ref in refs))
            parts.append(part)
        averages = member_means(parts[0] + parts[1] + parts[2] + parts[3], lower, 4 * features)
        average = blended(*averages, features - LANES)
        parts = [part - average for part in parts]
        squares = parts[0] * parts[0]
        for part in parts[1:]:
            squares = squares + part * part
        spreads = member_means(squares, lower, 4 * features)
        scale = blended(*(lax.rsqrt(spread + EPS) for spread in spreads), features - LANES)
        coarse = [None] * members
        for k, part in enumerate(parts):
            normed = (part * scale * gain_ref[k] + shift_ref[k]).astype(BF16)
            for member in range(members):
                term = padded_dot(window(normed, member), down_ref.at[k], member)
                coarse[member] = term if coarse[member] is None else coarse[member] + term
        coarse = jnp.concatenate(coarse, axis=0).astype(BF16)
        q = 1 - side
        lanes = slice(q * LANES, q * LANES + 2 * LANES)
        for p in range(2):
            grown = jnp.dot(coarse, up_ref[p, :, lanes], preferred_element_type=F32)
            squares = (grown * grown).astype(BF16)
            spread = jnp.dot(squares, sums[lanes, q * LANES : (q + 1) * LANES], preferred_element_type=F32)
            scale = lax.rsqrt(spread * (1.0 / features) + EPS)
            scale = jnp.concatenate([scale, scale], axis=-1)
            normed = grown * scale * up_gain_ref[:, lanes] + up_shift_ref[:, lanes]
            mixed = padded_dot(normed.astype(BF16), mix_ref, q)
            mixed = mixed.reshape(members, half_rows, levels, features)
            view = fine.at[side].reshape(members, half_rows, 2, levels, features)
            view[:, :, p] = mixed.astype(BF16)
        cleared(band_ref, fine.at[side])
        copy = pltpu.make_async_copy(
            fine.at[side, :, pl.ds(odd, slots)],
            out_ref.at[:, :, side * (columns - 1)],
            sem.at[side],
        )
        copy.start()
        copies.append(copy)
    for copy in copies:
        copy.wait()


def outer_of(band_rows, sides, gain, shift, down, up, up_gain, up_shift, mix, partial):
    members, slots, _, levels, features = partial.shape
    return pl.pallas_call(
        outer_kernel,
        out_shape=jax.ShapeDtypeStruct(partial.shape, BF16),
        in_specs=[SMEM] + [VMEM] * 11 + [HBM],
        out_specs=HBM,
        scratch_shapes=[
            pltpu.VMEM((2, members, slots + 2, levels, features), BF16),
            pltpu.SemaphoreType.DMA((2,)),
        ],
        input_output_aliases={12: 0},
        cost_estimate=cost(3 * 10**9, 10**6),
        compiler_params=room(12),
        name="outer",
    )(band_rows, *sides, gain, shift, down, up, up_gain, up_shift, mix, partial)


def assemble_kernel(*refs):
    pieces, (down_ref, up_ref) = refs[:-2], refs[-2:]
    pad = PAD // 8
    _, lat, up_tiles = up_ref.shape[1:4]
    own = pieces[0]
    tiles = own.shape[0] - 2 * up_tiles
    zero = jnp.zeros((pad,) + own.shape[1:], BF16)
    for part in range(down_ref.shape[0]):
        down_ref[part, :pad] = zero
        down_ref[part, pad + lat * tiles :] = zero
    here, place = lax.axis_index("lon"), lax.axis_index("lat")
    own, z1, z2, z3, core, across, across12, across3, rest, last = pieces
    far = lat - 1 - place
    beside = lax.bitwise_xor(place, 1)
    beside_far = lat - 1 - beside
    n = tiles + 2 * up_tiles
    table = [
        (own, 0, 0, place),
        (z1, 0, 1, place),
        (z2, 0, 2, place),
        (z3, 0, 3, place),
        (core, 0, 0, beside),
        (across, 0, 0, far),
        (across12, 0, 1, far),
        (across12, n, 2, far),
        (across3, 0, 3, far),
        (rest, 0, 1, beside),
        (rest, n, 2, beside),
        (rest, 2 * n, 3, beside),
        (rest, 3 * n, 0, beside_far),
        (rest, 4 * n, 1, beside_far),
        (rest, 5 * n, 2, beside_far),
        (last, 0, 3, beside_far),
    ]
    for ref, at, hop, row in table:
        source = lax.bitwise_xor(here, hop)
        down_ref[source, pl.ds(pad + row * tiles, tiles)] = ref[at : at + tiles]
        up_ref[0, source, row] = ref[at + tiles : at + tiles + up_tiles]
        up_ref[1, source, row] = ref[at + tiles + up_tiles : at + n]


def fast_weights(band_rows, tokens, down, up, features):
    lon, lat = lax.axis_size("lon"), lax.axis_size("lat")
    tiles, up_tiles = down.shape[0] // 8, up.shape[0] // 8
    place = lax.axis_index("lat")
    beside, mirror = lambda i: i ^ 1, lambda i: lat - 1 - i
    shard, core, across, west, east, tokens = first_sends(band_rows, tokens, down, up)
    core = swapped(core, "lat", beside)
    across = swapped(across, "lat", mirror)
    z2 = swapped(shard, "lon", lambda i: i ^ 2)
    z3 = swapped(shard, "lon", lambda i: i ^ 3)
    z1 = swapped(shard, "lon", beside)
    even = place % 2 == 0
    n = shard.shape[0]
    core_rows, across_rows = core[n:], across[n:]
    below = jnp.where(even, core_rows, across_rows)
    below = jnp.where(place == lat - 1, jnp.zeros_like(below), below)
    above = jnp.where(even, across_rows, core_rows)
    across12 = swapped(jnp.concatenate([z1, z2]), "lat", mirror)
    across3 = swapped(z3, "lat", mirror)
    rest = stacked([z1, z2, z3, across, across12], [n, n, n, n, 2 * n])
    rest = swapped(rest, "lat", beside)
    final = swapped(across3, "lat", beside)
    down, up = pl.pallas_call(
        assemble_kernel,
        out_shape=(
            jax.ShapeDtypeStruct((lon, lat * tiles + PAD // 4, 8, down.shape[1]), BF16),
            jax.ShapeDtypeStruct((2, lon, lat, up_tiles, 8, down.shape[1]), BF16),
        ),
        in_specs=[VMEM] * 10,
        out_specs=(VMEM,) * 2,
        compiler_params=room(6),
        name="assemble",
    )(shard, z1, z2, z3, core, across, across12, across3, rest, final)
    down = down.reshape(4, -1, down.shape[-1])
    return down, up, above, below, west, east, tokens


def plain_weights(band_rows, tokens, down, up, features):
    first, last = rows_of(band_rows, tokens)
    up = centred(up, features)
    below = passed_along(first, "lat", -1)
    above = passed_along(last, "lat", 1)
    rows, half = up.shape[0], up.shape[1] // 2
    shard = jnp.concatenate([down, up[:, :half], up[:, half:]], axis=0)
    whole = lax.all_gather(shard, ("lon", "lat"), axis=0)
    n = down.shape[0]
    up = jnp.stack([whole[:, n : n + rows], whole[:, n + rows :]])
    down = whole[:, :n].reshape(4, features, half)
    down = jnp.pad(down, ((0, 0), (PAD, PAD), (0, 0)))
    return down, up, above, below, *edges_of(band_rows, tokens), tokens


def whole(
    tokens, band_rows, down_gain, down_shift, down_weight, up_weight, up_gain, up_shift, mix_weight
):
    _, _, _, _, features = tokens.shape
    lon, lat = lax.axis_size("lon"), lax.axis_size("lat")
    block = tokens.transpose(0, 2, 3, 1, 4)
    plain = lon != 4 or lat != 4 or down_weight.shape[0] % 8 or up_weight.shape[0] % 8
    weights = plain_weights if plain else fast_weights
    results = weights(band_rows, block, down_weight, up_weight, features)
    down, up, above, below, west, east, near_by = results
    narrow = down_weight.shape[1]
    up = up.reshape(2, narrow, narrow)
    own_near, own_far = with_corners(band_rows, above, below, west, east)
    far = swapped(own_far, "lon", lambda i: (i - 1 if i % 2 == 0 else i + 1) % lon)
    near = swapped(own_near, "lon", lambda i: i ^ 1)
    gain, shift = down_gain.reshape(4, 1, features), down_shift.reshape(4, 1, features)
    twice = lambda value: jnp.concatenate([value, value], axis=-1)
    fine_gain, fine_shift = twice(up_gain)[None], twice(up_shift)[None]
    mix_weight = jnp.pad(mix_weight, ((PAD, PAD), (0, 0)))
    normed = inner_norm(band_rows, near_by, above, below, gain, shift)
    out = inner_of(
        band_rows, normed, down, up, fine_gain, fine_shift, mix_weight, block.shape
    )
    out = outer_of(
        band_rows,
        (near, far, own_near, own_far),
        twice(gain),
        twice(shift),
        down,
        up,
        fine_gain,
        fine_shift,
        mix_weight,
        out,
    )
    return out.transpose(0, 3, 1, 2, 4)


def solution(mesh):
    return jax.shard_map(
        whole,
        mesh=mesh,
        in_specs=(
            P("mem", None, "lat", "lon", None),
            P("lat", None),
            P(),
            P(),
            P(("lon", "lat"), None),
            P(("lon", "lat"), None),
            P(),
            P(),
            P(),
        ),
        out_specs=P("mem", None, "lat", "lon", None),
        check_vma=False,
    )
```
